32 devices in a mesh: group: 4 (over y, x), shard: 8 (over z, core).
Axes of the slice: x: 2, y: 2, z: 4, core: 2. Of those that a mesh axis runs over, the one named last changes fastest.
Arguments:
- embeddings: bfloat16 [128, 256, 768], P(('group', 'shard')), may hold values from -6 to 6
- assignments: int32 [128, 2, 256], P(('group', 'shard')), may hold values from 0 to 4095, as said below
- block_group: int32 [128], P(('group', 'shard')), may hold values from 0 to 3, as said below
- centroids: float32 [4, 4096, 768], P('group'), may hold values from -6 to 6
Outputs:
- subcentroids: float32 [4, 4096, 768], P('group', 'shard')
- inertia: float32 [4, 4096], P('group', 'shard')
The draws below stay inside these ranges and needn't reach their ends.
Inputs may be any that keep to these rules, and one draw needn't show every extreme that they name: `block_group`: of the 4 blocks of one device at most 2 name the same group; in every draw, for some group and some shard index, every device of that shard index has exactly 2 blocks naming that group. `assignments`: labels k with the same k // 512 form one range. In each block and iteration at most 64 rows have labels in one range; in every draw there is an iteration in which every block has exactly 64 rows in one common range.
All inputs are finite; a program needn't handle non-finite values.
Results may differ from the reference program's by a relative error of at most 0.0003.
Values may be sent and summed in bfloat16 or wider, within the bound.
A program may use at most 128 MiB of HBM per device.

```python
import jax
import jax.numpy as jnp

D = 768
K = 4096
BLOCK_ROWS = 256
ITERS = 2
BLK_DEV = 4
CAP = 2
BLOCKS = 128
MOST = 64
N_GROUP = 4
N_SHARD = 8


def draw_block_group(key, part):
    devices = BLOCKS // BLK_DEV
    pool_size = N_GROUP * CAP
    key_list = jax.random.split(jax.random.fold_in(key, 11), devices)
    ordering = jax.vmap(lambda subkey: jax.random.permutation(subkey, pool_size))(key_list)
    spread_out = (ordering[:, :BLK_DEV] % N_GROUP).astype(jnp.int32)
    rest_size = (N_GROUP - 1) * CAP
    key_other = jax.random.split(jax.random.fold_in(key, 12), devices)
    ordering_other = jax.vmap(lambda subkey: jax.random.permutation(subkey, rest_size))(key_other)
    target = jax.random.randint(jax.random.fold_in(key, 13), (), 0, N_GROUP).astype(jnp.int32)
    column = jax.random.randint(jax.random.fold_in(key, 14), (), 0, N_SHARD).astype(jnp.int32)
    others = ((target + 1 + ordering_other[:, :BLK_DEV - CAP] % (N_GROUP - 1)) % N_GROUP).astype(jnp.int32)
    crowded = jnp.concatenate([jnp.full((devices, CAP), target, jnp.int32), others], axis=1)
    chosen = jnp.arange(devices) % N_SHARD == column
    routing = jnp.where(chosen[:, None], crowded, spread_out)
    return routing.reshape(-1).astype(jnp.int32)


def draw_assignments(key, part):
    owned = K // N_SHARD
    cells = BLOCKS * ITERS
    pool_size = N_SHARD * MOST
    key_list = jax.random.split(jax.random.fold_in(key, 21), cells)
    spread_out = jax.vmap(lambda subkey: jax.random.permutation(subkey, pool_size)[:BLOCK_ROWS] % N_SHARD)(key_list)
    rest_size = (N_SHARD - 1) * MOST
    key_other = jax.random.split(jax.random.fold_in(key, 22), cells)
    other_part = jax.vmap(lambda subkey: jax.random.permutation(subkey, rest_size)[:BLOCK_ROWS - MOST] % (N_SHARD - 1))(key_other)
    target = jax.random.randint(jax.random.fold_in(key, 23), (), 0, N_SHARD).astype(jnp.int32)
    crowded = jnp.concatenate([jnp.full((cells, MOST), target, jnp.int32), ((target + 1 + other_part) % N_SHARD).astype(jnp.int32)], axis=1)
    key_mix = jax.random.split(jax.random.fold_in(key, 24), cells)
    crowded = jax.vmap(lambda subkey, row: row[jax.random.permutation(subkey, BLOCK_ROWS)])(key_mix, crowded)
    busy = jax.random.randint(jax.random.fold_in(key, 25), (), 0, ITERS).astype(jnp.int32)
    is_busy = jnp.arange(cells) % ITERS == busy
    range_ids = jnp.where(is_busy[:, None], crowded, spread_out).astype(jnp.int32)
    offsets = jax.random.randint(jax.random.fold_in(key, 26), (cells, BLOCK_ROWS), 0, owned).astype(jnp.int32)
    labels = range_ids * owned + offsets
    return labels.reshape(BLOCKS, ITERS, BLOCK_ROWS).astype(jnp.int32)


def steps_of(stream_key, shape, cuts, least, high):
    loudness, own = 1.0, jax.random.fold_in(stream_key, 6)
    for dim, parts in cuts:
        heights = jnp.exp(jax.random.uniform(jax.random.fold_in(own, dim), (parts,), jnp.float32, least / len(cuts), high / len(cuts)))
        loudness = loudness * jnp.repeat(heights, shape[dim] // parts).reshape([-1 if axis == dim else 1 for axis in range(len(shape))])
    return loudness


def normal_values(stream_key, extent, width, reach, cuts=(), held_as=jnp.bfloat16):
    level = steps_of(stream_key, extent, cuts, -0.22, 0.18) if cuts else 1.0
    entries = jax.random.normal(stream_key, extent, jnp.float32) * width * level
    return jnp.minimum(jnp.maximum(entries, -reach), reach).astype(held_as)


def setup_inputs(seed: int = 0) -> dict:
    arg_keys = jax.random.split(jax.random.key(seed), 5)
    embeddings = normal_values(arg_keys[0], (BLOCKS, BLOCK_ROWS, D), 1.0, 6.0, ((0, 32),))
    assignments = draw_assignments(jax.random.fold_in(arg_keys[4], 71), 0)
    block_group = draw_block_group(jax.random.fold_in(arg_keys[4], 71), 0)
    centroids = normal_values(arg_keys[3], (N_GROUP, K, D), 1.0, 6.0, ((0, 4),), jnp.float32)
    return dict(embeddings=embeddings, assignments=assignments, block_group=block_group, centroids=centroids)


PRIOR = 8.0


def reference(embeddings, assignments, block_group, centroids):
    block_count, block_rows, features = embeddings.shape
    groups, centers, unused = centroids.shape
    flat_rows = embeddings.reshape(-1, features).astype(jnp.float32)
    owners = jnp.repeat(block_group, block_rows).astype(jnp.int32)
    previous = centroids.reshape(groups * centers, features)
    inertia = jnp.zeros((groups * centers,), jnp.float32)
    for iteration in range(ITERS):
        labels = assignments[:, iteration, :].reshape(-1).astype(jnp.int32)
        segment = owners * centers + labels
        center_sums = jax.ops.segment_sum(flat_rows, segment, num_segments=groups * centers)
        counts = jax.ops.segment_sum(jnp.ones(labels.shape, jnp.float32), segment, num_segments=groups * centers)
        if iteration == ITERS - 1:
            difference = flat_rows - previous[segment]
            per_row = jnp.sum(difference * difference, axis=1)
            within = jax.ops.segment_sum(per_row, segment, num_segments=groups * centers)
            inertia = within / ((counts + PRIOR) * features)
        previous = (center_sums + PRIOR * previous) / (counts + PRIOR)[:, None]
    return previous.reshape(groups, centers, features), inertia.reshape(groups, centers)
```

```python
import functools

import jax
import jax.numpy as jnp
from jax import lax
from jax.experimental import pallas as pl
from jax.experimental.pallas import tpu as pltpu
from jax.sharding import PartitionSpec as P

PRIOR = 8.0
META = 8
CHUNKS = 3
MESH = pl.DeviceIdType.MESH


def exchange_kernel(n_gather, n_swap, width, column, *refs):
    n_in = n_gather + n_swap
    gathers, swaps = refs[:n_gather], refs[n_gather:n_in]
    outs = refs[n_in : 2 * n_in]
    gather_outs, swap_outs = outs[:n_gather], outs[n_gather:]
    scratch = refs[2 * n_in :]
    stages = scratch[:n_gather]
    scratch = scratch[n_gather:]

    groups, shards = lax.axis_size("group"), lax.axis_size("shard")
    chips = shards // 2
    mine, place = lax.axis_index("group"), lax.axis_index("shard")
    chip, core = place // 2, place % 2
    partner = (mine, chip * 2 + 1 - core)
    right = (mine, lax.rem(chip + 1, chips) * 2 + core)
    left = (mine, lax.rem(chip + chips - 1, chips) * 2 + core)

    def peer(step):
        return lax.rem(mine + step, groups)

    barrier = pltpu.get_barrier_semaphore()
    greeted = 0
    if n_gather:
        for device in (left, right, partner):
            pl.semaphore_signal(barrier, inc=1, device_id=device, device_id_type=MESH)
        greeted += 3
    if n_swap:
        for step in range(1, groups):
            pl.semaphore_signal(
                barrier, inc=1, device_id=(peer(step), place), device_id_type=MESH
            )
        greeted += groups - 1

    loads = []
    if n_gather:
        load_sem = scratch[0]
        for i in range(n_gather):
            source = gathers[i]
            if i == 0:
                source = source.at[:, :, pl.ds(column, width)]
            load = pltpu.make_async_copy(source, stages[i], load_sem.at[i])
            load.start()
            loads.append(load)
    pl.semaphore_wait(barrier, greeted)

    swap_copies = []
    if n_swap:
        swap_send, swap_recv = scratch[-2:]
        for step in range(1, groups):
            for i in range(n_swap):
                copy = pltpu.make_async_remote_copy(
                    src_ref=swaps[i].at[peer(step)],
                    dst_ref=swap_outs[i].at[step - 1],
                    send_sem=swap_send.at[i, step - 1],
                    recv_sem=swap_recv.at[i, step - 1],
                    device_id=(peer(step), place),
                    device_id_type=MESH,
                )
                copy.start()
                swap_copies.append(copy)

    if n_gather:
        store_sem, send_r, recv_r, send_l, recv_l, send_p, recv_p = scratch[1:8]
        stores = []

        def hop(i, source, origin, step, to, sends, recvs):
            return pltpu.make_async_remote_copy(
                src_ref=source,
                dst_ref=gather_outs[i].at[origin * 2 + core],
                send_sem=sends.at[i, step],
                recv_sem=recvs.at[i, step],
                device_id=to,
                device_id_type=MESH,
            )

        for i in range(n_gather):
            loads[i].wait()
            store = pltpu.make_async_copy(
                stages[i], gather_outs[i].at[place], store_sem.at[i]
            )

            @pl.when(chip < chips - 1)
            def _():
                hop(i, stages[i], chip, 0, right, send_r, recv_r).start()

            @pl.when(chip > 0)
            def _():
                hop(i, stages[i], chip, 0, left, send_l, recv_l).start()

            hop(i, stages[i], chip, chip, partner, send_p, recv_p).start()
            store.start()
            stores.append(store)

        for step in range(chips - 1):
            for i in range(n_gather):
                from_left = chip - 1 - step

                @pl.when(from_left >= 0)
                def _():
                    block = gather_outs[i].at[from_left * 2 + core]
                    hop(i, block, from_left, step, right, send_r, recv_r).wait_recv()

                    if step < chips - 2:

                        @pl.when(chip < chips - 1)
                        def _():
                            hop(i, block, from_left, step + 1, right, send_r, recv_r).start()

                    hop(i, block, from_left, from_left, partner, send_p, recv_p).start()

                from_right = chip + 1 + step

                @pl.when(from_right <= chips - 1)
                def _():
                    block = gather_outs[i].at[from_right * 2 + core]
                    hop(i, block, from_right, step, left, send_l, recv_l).wait_recv()

                    if step < chips - 2:

                        @pl.when(chip > 0)
                        def _():
                            hop(i, block, from_right, step + 1, left, send_l, recv_l).start()

                    hop(i, block, from_right, from_right, partner, send_p, recv_p).start()

        for i in range(n_gather):
            stores[i].wait()
            for step in range(chips - 1):

                @pl.when((chip - step >= 0) & (chip < chips - 1))
                def _():
                    hop(i, stages[i], chip, step, right, send_r, recv_r).wait_send()

                @pl.when((chip + step <= chips - 1) & (chip > 0))
                def _():
                    hop(i, stages[i], chip, step, left, send_l, recv_l).wait_send()

            for origin in range(chips):
                hop(i, stages[i], origin, origin, partner, send_p, recv_p).wait()

    for copy in swap_copies:
        copy.wait()


def exchange(gathers, swaps, width, column, key):
    groups, shards = lax.axis_size("group"), lax.axis_size("shard")
    chips = shards // 2
    n_gather, n_swap = len(gathers), len(swaps)
    shapes, scratch = [], []
    for i, array in enumerate(gathers):
        block = array.shape[:-1] + (width if i == 0 else array.shape[-1],)
        shapes.append(jax.ShapeDtypeStruct((shards,) + block, array.dtype))
        scratch.append(pltpu.VMEM(block, array.dtype))
    for array in swaps:
        shapes.append(jax.ShapeDtypeStruct((groups - 1,) + array.shape[1:], array.dtype))
    dma = pltpu.SemaphoreType.DMA
    if n_gather:
        scratch += [dma((n_gather,)), dma((n_gather,))]
        scratch += [dma((n_gather, max(chips - 1, 1)))] * 4
        scratch += [dma((n_gather, chips))] * 2
    if n_swap:
        scratch += [dma((n_swap, groups - 1))] * 2
    return pl.pallas_call(
        functools.partial(exchange_kernel, n_gather, n_swap, width, column),
        out_shape=shapes,
        in_specs=[pl.BlockSpec(memory_space=pl.ANY)] * (n_gather + n_swap),
        out_specs=[pl.BlockSpec(memory_space=pl.ANY)] * (n_gather + n_swap),
        scratch_shapes=scratch,
        compiler_params=pltpu.CompilerParams(collective_id=key, has_side_effects=True),
    )(*gathers, *swaps)


def tally_kernel(per_step, iters, with_extra, owners, labels, extra, rows, sums, *more):
    step = pl.program_id(0)
    centers = sums.shape[2]
    block_rows = rows.shape[1]

    @pl.when(step == 0)
    def _():
        sums[...] = jnp.zeros_like(sums)
        if with_extra:
            more[0][...] = jnp.zeros_like(more[0])

    ids = lax.broadcasted_iota(jnp.int32, (centers, block_rows), 0)
    for block in range(per_step):
        owner = owners[step * per_step + block]
        for t in range(iters):
            onehot = (ids == labels[block, t : t + 1, :]).astype(jnp.bfloat16)
            sums[owner, t] += jnp.dot(
                onehot, rows[block], preferred_element_type=jnp.float32
            )
            if with_extra:
                more[0][owner, t] += lax.dot_general(
                    extra[block],
                    onehot,
                    (((1,), (1,)), ((), ())),
                    preferred_element_type=jnp.float32,
                )


def tally(owners, labels, extra, rows, groups, centers, per_step, with_extra):
    blocks, iters, block_rows = labels.shape
    width = rows.shape[-1]
    shapes = [jax.ShapeDtypeStruct((groups, iters, centers, width), jnp.float32)]
    if with_extra:
        shapes.append(jax.ShapeDtypeStruct((groups, iters, extra.shape[1], centers), jnp.float32))
    out_specs = [pl.BlockSpec(s.shape, lambda i, o: (0, 0, 0, 0)) for s in shapes]
    return pl.pallas_call(
        functools.partial(tally_kernel, per_step, iters, with_extra),
        out_shape=shapes,
        grid_spec=pltpu.PrefetchScalarGridSpec(
            num_scalar_prefetch=1,
            grid=(blocks // per_step,),
            in_specs=[
                pl.BlockSpec((per_step, iters, block_rows), lambda i, o: (i, 0, 0)),
                pl.BlockSpec((per_step,) + extra.shape[1:], lambda i, o: (i, 0, 0)),
                pl.BlockSpec((per_step, block_rows, width), lambda i, o: (i, 0, 0)),
            ],
            out_specs=out_specs,
        ),
        compiler_params=pltpu.CompilerParams(vmem_limit_bytes=48 * 2**20),
    )(owners, labels, extra, rows)


def body(embeddings, assignments, block_group, centroids):
    groups, shards = lax.axis_size("group"), lax.axis_size("shard")
    mine, place = lax.axis_index("group"), lax.axis_index("shard")
    local, block_rows, features = embeddings.shape
    iters = assignments.shape[1]
    owned = centroids.shape[1] // shards
    chunks = CHUNKS if features % (CHUNKS * 128) == 0 else 1
    width = features // chunks
    blocks = shards * local

    wide = embeddings.astype(jnp.float32)
    squares = jnp.sum(wide * wide, axis=2)
    meta = jnp.concatenate(
        [
            assignments.astype(jnp.float32),
            jnp.broadcast_to(
                block_group[:, None, None].astype(jnp.float32), (local, 1, block_rows)
            ),
            squares[:, None, :],
            jnp.zeros((local, META - iters - 2, block_rows), jnp.float32),
        ],
        axis=1,
    )

    rows, metas = exchange([embeddings, meta], [], width, 0, 0)
    metas = metas.reshape(blocks, META, block_rows)
    labels = metas[:, :iters].astype(jnp.int32) - place * owned
    owners = metas[:, iters, 0].astype(jnp.int32)
    square = metas[:, iters + 1]
    high = lax.reduce_precision(square, 8, 7)
    middle = lax.reduce_precision(square - high, 8, 7)
    low = square - high - middle
    one = jnp.ones_like(square)
    zero = jnp.zeros_like(square)
    extra = jnp.stack([one, high, middle, low] + [zero] * 12, axis=1).astype(jnp.bfloat16)

    totals = []
    tail = None
    pending = []
    for chunk in range(chunks):
        result = tally(
            owners,
            labels,
            extra,
            rows.reshape(blocks, block_rows, width),
            groups,
            owned,
            local,
            chunk == 0,
        )
        column = (chunk + 1) * width
        if chunk + 1 < chunks:
            rows, *got = exchange([embeddings], result, width, column, chunk + 1)
        else:
            got = exchange([], result, width, 0, chunk + 1)
        whole = [
            lax.dynamic_index_in_dim(kept, mine, 0, keepdims=False) + jnp.sum(came, axis=0)
            for kept, came in zip(result, got)
        ]
        totals.append(whole[0])
        if chunk == 0:
            tail = whole[1]

    prior = lax.dynamic_slice_in_dim(centroids[0], place * owned, owned, 0)
    counts = tail[:, 0]
    within = tail[iters - 1, 1] + tail[iters - 1, 2] + tail[iters - 1, 3]
    pieces = []
    for chunk in range(chunks):
        previous = prior[:, chunk * width : (chunk + 1) * width]
        for t in range(iters):
            sums = totals[chunk][t]
            count = counts[t][:, None]
            if t == iters - 1:
                within = within + jnp.sum(
                    previous * (count * previous - 2.0 * sums), axis=1
                )
            previous = (sums + PRIOR * previous) / (count + PRIOR)
        pieces.append(previous)
    inertia = within / ((counts[iters - 1] + PRIOR) * features)
    return (jnp.concatenate(pieces, axis=1)[None], inertia[None])


LANES = 128
META_ROWS = 16
FIXED = 6
LEVELS = 32000.0
HALF = 32768.0


def fused_kernel(
    chunks, most, meta_in, emb, cents, out, inertia,
    rows, metas, select, place_in, acc, compact, own, send, recv, inv, scale, cnt, ext,
    ext_recv, prior, result, within,
    load_sem, misc_sem, prior_sem, out_sem, meta_send, meta_recv, metap_send, metap_recv,
    send_r, recv_r, send_l, recv_l, send_p, recv_p, ext_ssem, ext_rsem, swap_send, swap_recv,
):
    groups, shards = lax.axis_size("group"), lax.axis_size("shard")
    chips = shards // 2
    mine, place = lax.axis_index("group"), lax.axis_index("shard")
    chip, core = place // 2, place % 2
    partner = (mine, chip * 2 + 1 - core)
    right, left = (mine, place + 2), (mine, place - 2)
    local, block_rows, features = emb.shape
    width = rows.shape[-1]
    iters = place_in.shape[0]
    owned = own.shape[2]
    slots = local * most
    reps = owned // LANES

    def peer(step):
        return (lax.rem(mine + step, groups), place)

    def remote(src, dst, ssem, rsem, to):
        return pltpu.make_async_remote_copy(
            src_ref=src, dst_ref=dst, send_sem=ssem, recv_sem=rsem,
            device_id=to, device_id_type=MESH,
        )

    def load(c):
        return pltpu.make_async_copy(
            emb.at[:, :, pl.ds(pl.multiple_of(c * width, width), width)],
            rows.at[c, place], load_sem.at[c],
        )

    def load_prior(c):
        return pltpu.make_async_copy(
            cents.at[0, pl.ds(pl.multiple_of(place * owned, owned), owned),
                     pl.ds(pl.multiple_of(c * width, width), width)],
            prior.at[c], prior_sem.at[c],
        )

    meta_load = pltpu.make_async_copy(meta_in, metas.at[place], misc_sem.at[0])
    meta_load.start()
    for c in range(chunks):
        load(c).start()

    barrier = pltpu.get_barrier_semaphore()
    for other in range(1, chips):
        pl.semaphore_signal(
            barrier, inc=1, device_id=(mine, lax.rem(chip + other, chips) * 2 + core),
            device_id_type=MESH,
        )
    pl.semaphore_signal(barrier, inc=1, device_id=partner, device_id_type=MESH)
    for step in range(1, groups):
        pl.semaphore_signal(barrier, inc=1, device_id=peer(step), device_id_type=MESH)
    pl.semaphore_wait(barrier, chips + groups - 1)

    def meta_to(other):
        target = lax.rem(chip + other, chips)
        return remote(
            metas.at[place], metas.at[place], meta_send.at[other], meta_recv.at[other],
            (mine, target * 2 + core),
        )

    def meta_partner(q):
        block = metas.at[q * 2 + core]
        return remote(block, block, metap_send.at[q], metap_recv.at[q], partner)

    meta_load.wait()
    for other in range(1, chips):
        meta_to(other).start()

    def to_right(c, q):
        block = rows.at[c, q * 2 + core]
        return remote(block, block, send_r.at[c, chip - q], recv_r.at[c, chip - q], right)

    def to_left(c, q):
        block = rows.at[c, q * 2 + core]
        return remote(block, block, send_l.at[c, q - chip], recv_l.at[c, q - chip], left)

    def to_partner(c, q):
        block = rows.at[c, q * 2 + core]
        return remote(block, block, send_p.at[c, q], recv_p.at[c, q], partner)

    def from_left(c, q):
        block = rows.at[c, q * 2 + core]
        return remote(
            block, block, send_r.at[c, chip - 1 - q], recv_r.at[c, chip - 1 - q], right
        )

    def from_right(c, q):
        block = rows.at[c, q * 2 + core]
        return remote(
            block, block, send_l.at[c, q - chip - 1], recv_l.at[c, q - chip - 1], left
        )

    def from_partner(c, q):
        block = rows.at[c, q * 2 + 1 - core]
        return remote(block, block, send_p.at[c, q], recv_p.at[c, q], partner)

    def issue_own(c):
        load(c).wait()

        @pl.when(chip < chips - 1)
        def _():
            to_right(c, chip).start()

        @pl.when(chip > 0)
        def _():
            to_left(c, chip).start()

        to_partner(c, chip).start()

    issue_own(0)
    issue_own(1)
    for c in range(chunks):
        load_prior(c).start()

    on_left, on_right = chip, chips - 1 - chip
    both = jnp.minimum(on_left, on_right)

    def source(k):
        paired = k <= 2 * both
        distance = jnp.where(paired, (k + 1) // 2, k - both)
        is_left = jnp.where(paired, (k % 2) == 1, on_left > on_right)
        return jnp.where(is_left, chip - distance, chip + distance)

    ids_r = lax.broadcasted_iota(jnp.int32, (slots, block_rows), 0)
    ids_c = lax.broadcasted_iota(jnp.int32, (owned, slots), 0)

    ext[...] = jnp.zeros_like(ext)
    acc[...] = jnp.zeros_like(acc)

    def take_meta(q, core_of):
        origin = q * 2 + core_of
        for t in range(iters):
            base = FIXED + 4 * t
            wide = jnp.zeros((META_ROWS, slots), jnp.float32)
            for b in range(local):
                e = metas[origin, b]
                f = e.astype(jnp.float32)
                wanted = f[base + 2 : base + 3, :].astype(jnp.int32) == place
                pos = jnp.where(wanted, f[base + 3 : base + 4, :].astype(jnp.int32) + b * most, -1)
                hot = (ids_r == pos).astype(jnp.bfloat16)
                select[origin, b, t * most : (t + 1) * most, :] = hot[b * most : (b + 1) * most, :]
                wide = wide + lax.dot_general(
                    e, hot, (((1,), (1,)), ((), ())), preferred_element_type=jnp.float32
                )
            step = wide[5:6, :].astype(jnp.int32) - mine
            step = jnp.where(step < 0, step + groups, step)
            label = wide[base : base + 1, :] + 256.0 * wide[base + 1 : base + 2, :]
            cell = jnp.where(wide[0:1, :] > 0.5, step * owned + label.astype(jnp.int32), -1)
            packed = wide.astype(jnp.bfloat16)
            for g in range(groups):
                hot = (ids_c == cell - g * owned).astype(jnp.bfloat16)
                place_in[t, q, g * owned : (g + 1) * owned, core_of * slots : (core_of + 1) * slots] = hot
                ext[g, t] += lax.dot_general(
                    packed, hot, (((1,), (1,)), ((), ())), preferred_element_type=jnp.float32
                )

    def meta_step(k, carry):
        q = source(k)

        @pl.when(q != chip)
        def _():
            other = lax.rem(chip - q + chips, chips)
            block = metas.at[q * 2 + core]
            remote(block, block, meta_send.at[other], meta_recv.at[other], left).wait_recv()

        meta_partner(q).start()
        for core_of in range(2):

            @pl.when(core_of != core)
            def _():
                block = metas.at[q * 2 + 1 - core]
                remote(block, block, metap_send.at[q], metap_recv.at[q], partner).wait_recv()

        for core_of in range(2):
            take_meta(q, core_of)
        return carry

    lax.fori_loop(0, chips, meta_step, 0)

    def ext_to(step):
        return remote(
            ext.at[step], ext_recv.at[step - 1], ext_ssem.at[step - 1], ext_rsem.at[step - 1],
            peer(step),
        )

    for step in range(1, groups):
        ext_to(step).start()

    def tall(row):
        return jnp.broadcast_to(row, (LANES, LANES)).T

    for step in range(1, groups):
        for t in range(iters):
            for i in range(reps):
                bound = ext[step, t, 4:5, i * LANES : (i + 1) * LANES]
                inv[step - 1, t, i * LANES : (i + 1) * LANES, :] = tall(
                    LEVELS / jnp.maximum(bound, 1e-30)
                )

    def swap(c, step):
        return remote(
            send.at[c, step - 1], recv.at[c, step - 1], swap_send.at[c, step - 1],
            swap_recv.at[c, step - 1], peer(step),
        )

    tile = owned

    def tally(c, q, first):
        for core_of in range(2):
            origin = q * 2 + core_of
            for b in range(local):
                got = jnp.dot(
                    select[origin, b], rows[c, origin, b], preferred_element_type=jnp.float32
                ).astype(jnp.bfloat16)
                for t in range(iters):
                    compact[t, core_of * slots + b * most : core_of * slots + (b + 1) * most, :] = got[
                        t * most : (t + 1) * most, :
                    ]

        def body(i, carry):
            for t in range(iters):
                part = pl.ds(pl.multiple_of(i * tile, tile), tile)
                acc[t, part, :] += jnp.dot(
                    place_in[t, q, part, :], compact[t], preferred_element_type=jnp.float32
                )
            return carry

        lax.fori_loop(0, groups, body, 0)

    def settle(c):
        for t in range(iters):
            own[c, t] = acc[t, :owned, :]
        for step in range(1, groups):
            part = slice(step * owned, (step + 1) * owned)
            high = (acc[0, part, :] * inv[step - 1, 0] + (HALF + 0.5)).astype(jnp.int32)
            low = (acc[1, part, :] * inv[step - 1, 1] + (HALF + 0.5)).astype(jnp.int32)
            send[c, step - 1] = (high << 16) | low
            swap(c, step).start()
        acc[...] = jnp.zeros_like(acc)

    def scales():
        for step in range(1, groups):
            ext_to(step).wait_recv()
        for t in range(iters):
            for i in range(reps):
                part = slice(i * LANES, (i + 1) * LANES)
                count = ext[0, t, 0:1, part]
                for step in range(1, groups):
                    count = count + ext_recv[step - 1, t, 0:1, part]
                    scale[step - 1, t, part, :] = tall(ext_recv[step - 1, t, 4:5, part] / LEVELS)
                cnt[t, part, :] = tall(count)
        within[...] = jnp.zeros_like(within)

    def finish(c):
        load_prior(c).wait()
        for step in range(1, groups):
            swap(c, step).wait_recv()
        for i in range(reps):
            part = slice(i * LANES, (i + 1) * LANES)
            sums = [own[c, t, part, :] for t in range(iters)]
            for step in range(1, groups):
                word = recv[c, step - 1, part, :]
                high = lax.shift_right_logical(word, 16)
                low = word & 0xFFFF
                for t, code in enumerate((high, low)):
                    sums[t] = sums[t] + (code.astype(jnp.float32) - HALF) * scale[step - 1, t, part, :]
            previous = prior[c, part, :]
            for t in range(iters):
                count = cnt[t, part, :]
                if t == iters - 1:
                    within[part, :] += previous * (count * previous - 2.0 * sums[t])
                previous = (sums[t] + PRIOR * previous) / (count + PRIOR)
            result[c, part, :] = previous

    def store(c):
        return pltpu.make_async_copy(
            result.at[c], out.at[:, pl.ds(pl.multiple_of(c * width, width), width)], out_sem.at[c]
        )

    def main_step(j, carry):
        c, k = j // chips, j % chips
        q = source(k)

        @pl.when((k == 0) & (c + 2 < chunks))
        def _():
            issue_own(c + 2)

        @pl.when(q < chip)
        def _():
            from_left(c, q).wait_recv()

            @pl.when(chip < chips - 1)
            def _():
                to_right(c, q).start()

            to_partner(c, q).start()

        @pl.when(q > chip)
        def _():
            from_right(c, q).wait_recv()

            @pl.when(chip > 0)
            def _():
                to_left(c, q).start()

            to_partner(c, q).start()

        from_partner(c, q).wait_recv()
        tally(c, q, k == 0)

        @pl.when(k == chips - 1)
        def _():
            settle(c)

            @pl.when(c == 0)
            def _():
                scales()

            @pl.when(c > 0)
            def _():
                finish(c - 1)
                store(c - 1).start()

        return carry

    lax.fori_loop(0, chunks * chips, main_step, 0)
    finish(chunks - 1)
    store(chunks - 1).start()

    for i in range(reps):
        part = slice(i * LANES, (i + 1) * LANES)
        spread = jnp.sum(within[part, :].T, axis=0, keepdims=True)
        last = iters - 1
        count = ext[0, last, 0:1, part]
        square = ext[0, last, 1:2, part] + ext[0, last, 2:3, part] + ext[0, last, 3:4, part]
        for step in range(1, groups):
            far = ext_recv[step - 1, last, :, part]
            count = count + far[0:1]
            square = square + far[1:2] + far[2:3] + far[3:4]
        inertia[:, part] = (spread + square) / ((count + PRIOR) * features)

    for other in range(1, chips):
        meta_to(other).wait_send()
    for q in range(chips):
        meta_partner(q).wait_send()
    for step in range(1, groups):
        ext_to(step).wait_send()

    def drain(j, carry):
        c, q = j // chips, j % chips

        @pl.when((q <= chip) & (chip < chips - 1))
        def _():
            to_right(c, q).wait_send()

        @pl.when((q >= chip) & (chip > 0))
        def _():
            to_left(c, q).wait_send()

        to_partner(c, q).wait_send()
        return carry

    lax.fori_loop(0, chunks * chips, drain, 0)
    for c in range(chunks):
        for step in range(1, groups):
            swap(c, step).wait_send()
        store(c).wait()


def fused_buffers(local, block_rows, features, iters, owned, groups, shards):
    chips = shards // 2
    most = 2 * block_rows // shards
    width, chunks = LANES, features // LANES
    slots = local * most
    vmem = pltpu.VMEM
    f32, b16, i32 = jnp.float32, jnp.bfloat16, jnp.int32
    buffers = [
        ((chunks, shards, local, block_rows, width), b16),
        ((shards, local, META_ROWS, block_rows), b16),
        ((shards, local, iters * most, block_rows), b16),
        ((iters, chips, groups * owned, 2 * slots), b16),
        ((iters, groups * owned, width), f32),
        ((iters, 2 * slots, width), b16),
        ((chunks, iters, owned, width), f32),
        ((chunks, groups - 1, owned, width), i32),
        ((chunks, groups - 1, owned, width), i32),
        ((groups - 1, iters, owned, width), f32),
        ((groups - 1, iters, owned, width), f32),
        ((iters, owned, width), f32),
        ((groups, iters, META_ROWS, owned), f32),
        ((groups - 1, iters, META_ROWS, owned), f32),
        ((chunks, owned, width), f32),
        ((chunks, owned, width), f32),
        ((owned, width), f32),
    ]
    dma = pltpu.SemaphoreType.DMA
    sems = [dma((chunks,)), dma((1,)), dma((chunks,)), dma((chunks,))]
    sems += [dma((chips,))] * 4
    sems += [dma((chunks, chips))] * 6
    sems += [dma((groups - 1,))] * 2
    sems += [dma((chunks, groups - 1))] * 2
    return [vmem(s, d) for s, d in buffers], sems, buffers, most, chunks


def fits(local, block_rows, features, iters, owned, groups, shards):
    if features % LANES or features < 2 * LANES or owned % LANES or shards % 2:
        return False
    if iters != 2 or 4 * iters + FIXED > META_ROWS or (2 * block_rows) % shards:
        return False
    most = 2 * block_rows // shards
    if (local * most) % LANES or most % 16 or block_rows % LANES:
        return False
    total = 0
    for shape, dtype in fused_buffers(local, block_rows, features, iters, owned, groups, shards)[2]:
        size = jnp.dtype(dtype).itemsize
        for extent in shape:
            size *= extent
        total += size
    return total < 58 * 2**20


def fused_body(embeddings, assignments, block_group, centroids):
    groups, shards = lax.axis_size("group"), lax.axis_size("shard")
    local, block_rows, features = embeddings.shape
    iters = assignments.shape[1]
    owned = centroids.shape[1] // shards
    buffers, sems, unused, most, chunks = fused_buffers(
        local, block_rows, features, iters, owned, groups, shards
    )

    wide = embeddings.astype(jnp.float32)
    square = jnp.sum(wide * wide, axis=2)
    peak = jnp.max(jnp.abs(wide), axis=2)
    high = lax.reduce_precision(square, 8, 7)
    middle = lax.reduce_precision(square - high, 8, 7)
    low = square - high - middle
    ranges = assignments // owned
    inside = (assignments % owned)
    hot = (ranges[:, :, None, :] == jnp.arange(shards)[:, None]).astype(jnp.bfloat16)
    before = (jnp.arange(block_rows)[:, None] < jnp.arange(block_rows)[None, :]).astype(jnp.bfloat16)
    earlier = jnp.dot(hot.reshape(-1, block_rows), before, preferred_element_type=jnp.float32)
    rank = jnp.sum(earlier.reshape(hot.shape) * hot.astype(jnp.float32), axis=2)
    one = jnp.ones_like(square)
    owner = jnp.broadcast_to(block_group[:, None].astype(jnp.float32), square.shape)
    lines = [one, high, middle, low, peak, owner]
    for t in range(iters):
        lines += [
            (inside[:, t] % 256).astype(jnp.float32),
            (inside[:, t] // 256).astype(jnp.float32),
            ranges[:, t].astype(jnp.float32),
            rank[:, t],
        ]
    lines += [jnp.zeros_like(square)] * (META_ROWS - len(lines))
    meta = jnp.stack(lines, axis=1).astype(jnp.bfloat16)

    out, inertia = pl.pallas_call(
        functools.partial(fused_kernel, chunks, most),
        out_shape=[
            jax.ShapeDtypeStruct((owned, features), jnp.float32),
            jax.ShapeDtypeStruct((1, owned), jnp.float32),
        ],
        in_specs=[pl.BlockSpec(memory_space=pl.ANY)] * 3,
        out_specs=[
            pl.BlockSpec(memory_space=pl.ANY),
            pl.BlockSpec(memory_space=pltpu.VMEM),
        ],
        scratch_shapes=buffers + sems,
        compiler_params=pltpu.CompilerParams(
            collective_id=0, has_side_effects=True, vmem_limit_bytes=63 * 2**20
        ),
    )(meta, embeddings, centroids)
    return out[None], inertia


def choose(embeddings, assignments, block_group, centroids):
    groups, shards = lax.axis_size("group"), lax.axis_size("shard")
    local, block_rows, features = embeddings.shape
    owned = centroids.shape[1] // shards
    if fits(local, block_rows, features, assignments.shape[1], owned, groups, shards):
        return fused_body(embeddings, assignments, block_group, centroids)
    return body(embeddings, assignments, block_group, centroids)


def solution(mesh):
    in_specs = (
        P(("group", "shard"), None, None),
        P(("group", "shard"), None, None),
        P(("group", "shard")),
        P("group", None, None),
    )
    out_specs = (P("group", "shard", None), P("group", "shard"))
    return jax.shard_map(choose, mesh=mesh, in_specs=in_specs, out_specs=out_specs, check_vma=False)
```

```python
import functools

import jax
import jax.numpy as jnp
from jax import lax
from jax.experimental import pallas as pl
from jax.experimental.pallas import tpu as pltpu
from jax.sharding import PartitionSpec as P

PRIOR = 8.0
META = 8
CHUNKS = 3
MESH = pl.DeviceIdType.MESH


def exchange_kernel(n_gather, n_swap, width, column, *refs):
    n_in = n_gather + n_swap
    gathers, swaps = refs[:n_gather], refs[n_gather:n_in]
    outs = refs[n_in : 2 * n_in]
    gather_outs, swap_outs = outs[:n_gather], outs[n_gather:]
    scratch = refs[2 * n_in :]
    stages = scratch[:n_gather]
    scratch = scratch[n_gather:]

    groups, shards = lax.axis_size("group"), lax.axis_size("shard")
    chips = shards // 2
    mine, place = lax.axis_index("group"), lax.axis_index("shard")
    chip, core = place // 2, place % 2
    partner = (mine, chip * 2 + 1 - core)
    right = (mine, lax.rem(chip + 1, chips) * 2 + core)
    left = (mine, lax.rem(chip + chips - 1, chips) * 2 + core)

    def peer(step):
        return lax.rem(mine + step, groups)

    barrier = pltpu.get_barrier_semaphore()
    greeted = 0
    if n_gather:
        for device in (left, right, partner):
            pl.semaphore_signal(barrier, inc=1, device_id=device, device_id_type=MESH)
        greeted += 3
    if n_swap:
        for step in range(1, groups):
            pl.semaphore_signal(
                barrier, inc=1, device_id=(peer(step), place), device_id_type=MESH
            )
        greeted += groups - 1

    loads = []
    if n_gather:
        load_sem = scratch[0]
        for i in range(n_gather):
            source = gathers[i]
            if i == 0:
                source = source.at[:, :, pl.ds(column, width)]
            load = pltpu.make_async_copy(source, stages[i], load_sem.at[i])
            load.start()
            loads.append(load)
    pl.semaphore_wait(barrier, greeted)

    swap_copies = []
    if n_swap:
        swap_send, swap_recv = scratch[-2:]
        for step in range(1, groups):
            for i in range(n_swap):
                copy = pltpu.make_async_remote_copy(
                    src_ref=swaps[i].at[peer(step)],
                    dst_ref=swap_outs[i].at[step - 1],
                    send_sem=swap_send.at[i, step - 1],
                    recv_sem=swap_recv.at[i, step - 1],
                    device_id=(peer(step), place),
                    device_id_type=MESH,
                )
                copy.start()
                swap_copies.append(copy)

    if n_gather:
        store_sem, send_r, recv_r, send_l, recv_l, send_p, recv_p = scratch[1:8]
        stores = []

        def hop(i, source, origin, step, to, sends, recvs):
            return pltpu.make_async_remote_copy(
                src_ref=source,
                dst_ref=gather_outs[i].at[origin * 2 + core],
                send_sem=sends.at[i, step],
                recv_sem=recvs.at[i, step],
                device_id=to,
                device_id_type=MESH,
            )

        for i in range(n_gather):
            loads[i].wait()
            store = pltpu.make_async_copy(
                stages[i], gather_outs[i].at[place], store_sem.at[i]
            )

            @pl.when(chip < chips - 1)
            def _():
                hop(i, stages[i], chip, 0, right, send_r, recv_r).start()

            @pl.when(chip > 0)
            def _():
                hop(i, stages[i], chip, 0, left, send_l, recv_l).start()

            hop(i, stages[i], chip, chip, partner, send_p, recv_p).start()
            store.start()
            stores.append(store)

        for step in range(chips - 1):
            for i in range(n_gather):
                from_left = chip - 1 - step

                @pl.when(from_left >= 0)
                def _():
                    block = gather_outs[i].at[from_left * 2 + core]
                    hop(i, block, from_left, step, right, send_r, recv_r).wait_recv()

                    if step < chips - 2:

                        @pl.when(chip < chips - 1)
                        def _():
                            hop(i, block, from_left, step + 1, right, send_r, recv_r).start()

                    hop(i, block, from_left, from_left, partner, send_p, recv_p).start()

                from_right = chip + 1 + step

                @pl.when(from_right <= chips - 1)
                def _():
                    block = gather_outs[i].at[from_right * 2 + core]
                    hop(i, block, from_right, step, left, send_l, recv_l).wait_recv()

                    if step < chips - 2:

                        @pl.when(chip > 0)
                        def _():
                            hop(i, block, from_right, step + 1, left, send_l, recv_l).start()

                    hop(i, block, from_right, from_right, partner, send_p, recv_p).start()

        for i in range(n_gather):
            stores[i].wait()
            for step in range(chips - 1):

                @pl.when((chip - step >= 0) & (chip < chips - 1))
                def _():
                    hop(i, stages[i], chip, step, right, send_r, recv_r).wait_send()

                @pl.when((chip + step <= chips - 1) & (chip > 0))
                def _():
                    hop(i, stages[i], chip, step, left, send_l, recv_l).wait_send()

            for origin in range(chips):
                hop(i, stages[i], origin, origin, partner, send_p, recv_p).wait()

    for copy in swap_copies:
        copy.wait()


def exchange(gathers, swaps, width, column, key):
    groups, shards = lax.axis_size("group"), lax.axis_size("shard")
    chips = shards // 2
    n_gather, n_swap = len(gathers), len(swaps)
    shapes, scratch = [], []
    for i, array in enumerate(gathers):
        block = array.shape[:-1] + (width if i == 0 else array.shape[-1],)
        shapes.append(jax.ShapeDtypeStruct((shards,) + block, array.dtype))
        scratch.append(pltpu.VMEM(block, array.dtype))
    for array in swaps:
        shapes.append(jax.ShapeDtypeStruct((groups - 1,) + array.shape[1:], array.dtype))
    dma = pltpu.SemaphoreType.DMA
    if n_gather:
        scratch += [dma((n_gather,)), dma((n_gather,))]
        scratch += [dma((n_gather, max(chips - 1, 1)))] * 4
        scratch += [dma((n_gather, chips))] * 2
    if n_swap:
        scratch += [dma((n_swap, groups - 1))] * 2
    return pl.pallas_call(
        functools.partial(exchange_kernel, n_gather, n_swap, width, column),
        out_shape=shapes,
        in_specs=[pl.BlockSpec(memory_space=pl.ANY)] * (n_gather + n_swap),
        out_specs=[pl.BlockSpec(memory_space=pl.ANY)] * (n_gather + n_swap),
        scratch_shapes=scratch,
        compiler_params=pltpu.CompilerParams(collective_id=key, has_side_effects=True),
    )(*gathers, *swaps)


def tally_kernel(per_step, iters, with_extra, owners, labels, extra, rows, sums, *more):
    step = pl.program_id(0)
    centers = sums.shape[2]
    block_rows = rows.shape[1]

    @pl.when(step == 0)
    def _():
        sums[...] = jnp.zeros_like(sums)
        if with_extra:
            more[0][...] = jnp.zeros_like(more[0])

    ids = lax.broadcasted_iota(jnp.int32, (centers, block_rows), 0)
    for block in range(per_step):
        owner = owners[step * per_step + block]
        for t in range(iters):
            onehot = (ids == labels[block, t : t + 1, :]).astype(jnp.bfloat16)
            sums[owner, t] += jnp.dot(
                onehot, rows[block], preferred_element_type=jnp.float32
            )
            if with_extra:
                more[0][owner, t] += lax.dot_general(
                    extra[block],
                    onehot,
                    (((1,), (1,)), ((), ())),
                    preferred_element_type=jnp.float32,
                )


def tally(owners, labels, extra, rows, groups, centers, per_step, with_extra):
    blocks, iters, block_rows = labels.shape
    width = rows.shape[-1]
    shapes = [jax.ShapeDtypeStruct((groups, iters, centers, width), jnp.float32)]
    if with_extra:
        shapes.append(jax.ShapeDtypeStruct((groups, iters, extra.shape[1], centers), jnp.float32))
    out_specs = [pl.BlockSpec(s.shape, lambda i, o: (0, 0, 0, 0)) for s in shapes]
    return pl.pallas_call(
        functools.partial(tally_kernel, per_step, iters, with_extra),
        out_shape=shapes,
        grid_spec=pltpu.PrefetchScalarGridSpec(
            num_scalar_prefetch=1,
            grid=(blocks // per_step,),
            in_specs=[
                pl.BlockSpec((per_step, iters, block_rows), lambda i, o: (i, 0, 0)),
                pl.BlockSpec((per_step,) + extra.shape[1:], lambda i, o: (i, 0, 0)),
                pl.BlockSpec((per_step, block_rows, width), lambda i, o: (i, 0, 0)),
            ],
            out_specs=out_specs,
        ),
        compiler_params=pltpu.CompilerParams(vmem_limit_bytes=48 * 2**20),
    )(owners, labels, extra, rows)


def body(embeddings, assignments, block_group, centroids):
    groups, shards = lax.axis_size("group"), lax.axis_size("shard")
    mine, place = lax.axis_index("group"), lax.axis_index("shard")
    local, block_rows, features = embeddings.shape
    iters = assignments.shape[1]
    owned = centroids.shape[1] // shards
    chunks = CHUNKS if features % (CHUNKS * 128) == 0 else 1
    width = features // chunks
    blocks = shards * local

    wide = embeddings.astype(jnp.float32)
    squares = jnp.sum(wide * wide, axis=2)
    meta = jnp.concatenate(
        [
            assignments.astype(jnp.float32),
            jnp.broadcast_to(
                block_group[:, None, None].astype(jnp.float32), (local, 1, block_rows)
            ),
            squares[:, None, :],
            jnp.zeros((local, META - iters - 2, block_rows), jnp.float32),
        ],
        axis=1,
    )

    rows, metas = exchange([embeddings, meta], [], width, 0, 0)
    metas = metas.reshape(blocks, META, block_rows)
    labels = metas[:, :iters].astype(jnp.int32) - place * owned
    owners = metas[:, iters, 0].astype(jnp.int32)
    square = metas[:, iters + 1]
    high = lax.reduce_precision(square, 8, 7)
    middle = lax.reduce_precision(square - high, 8, 7)
    low = square - high - middle
    one = jnp.ones_like(square)
    zero = jnp.zeros_like(square)
    extra = jnp.stack([one, high, middle, low] + [zero] * 12, axis=1).astype(jnp.bfloat16)

    totals = []
    tail = None
    pending = []
    for chunk in range(chunks):
        result = tally(
            owners,
            labels,
            extra,
            rows.reshape(blocks, block_rows, width),
            groups,
            owned,
            local,
            chunk == 0,
        )
        column = (chunk + 1) * width
        if chunk + 1 < chunks:
            rows, *got = exchange([embeddings], result, width, column, chunk + 1)
        else:
            got = exchange([], result, width, 0, chunk + 1)
        whole = [
            lax.dynamic_index_in_dim(kept, mine, 0, keepdims=False) + jnp.sum(came, axis=0)
            for kept, came in zip(result, got)
        ]
        totals.append(whole[0])
        if chunk == 0:
            tail = whole[1]

    prior = lax.dynamic_slice_in_dim(centroids[0], place * owned, owned, 0)
    counts = tail[:, 0]
    within = tail[iters - 1, 1] + tail[iters - 1, 2] + tail[iters - 1, 3]
    pieces = []
    for chunk in range(chunks):
        previous = prior[:, chunk * width : (chunk + 1) * width]
        for t in range(iters):
            sums = totals[chunk][t]
            count = counts[t][:, None]
            if t == iters - 1:
                within = within + jnp.sum(
                    previous * (count * previous - 2.0 * sums), axis=1
                )
            previous = (sums + PRIOR * previous) / (count + PRIOR)
        pieces.append(previous)
    inertia = within / ((counts[iters - 1] + PRIOR) * features)
    return (jnp.concatenate(pieces, axis=1)[None], inertia[None])


LANES = 128
META_ROWS = 16
FIXED = 6
LEVELS = 32000.0
HALF = 32768.0


def fused_kernel(
    chunks, most, owner_in, label_in, emb, cents, out, inertia,
    rows, metas, select, place_in, acc, compact, own, send, recv, inv, scale, cnt, ext,
    ext_recv, prior, within, lines,
    load_sem, prior_sem, meta_send, meta_recv, metap_send, metap_recv,
    send_r, recv_r, send_l, recv_l, send_p, recv_p, ext_ssem, ext_rsem, swap_send, swap_recv,
):
    groups, shards = lax.axis_size("group"), lax.axis_size("shard")
    chips = shards // 2
    mine, place = lax.axis_index("group"), lax.axis_index("shard")
    chip, core = place // 2, place % 2
    partner = (mine, chip * 2 + 1 - core)
    right, left = (mine, place + 2), (mine, place - 2)
    local, block_rows, features = emb.shape
    width = rows.shape[-1]
    iters = place_in.shape[0]
    owned = own.shape[2]
    slots = local * most
    reps = owned // LANES

    def peer(step):
        return (lax.rem(mine + step, groups), place)

    def remote(src, dst, ssem, rsem, to):
        return pltpu.make_async_remote_copy(
            src_ref=src, dst_ref=dst, send_sem=ssem, recv_sem=rsem,
            device_id=to, device_id_type=MESH,
        )

    def load(c):
        return pltpu.make_async_copy(
            emb.at[:, :, pl.ds(pl.multiple_of(c * width, width), width)],
            rows.at[c, place], load_sem.at[c],
        )

    def load_prior(c):
        return pltpu.make_async_copy(
            cents.at[0, pl.ds(pl.multiple_of(place * owned, owned), owned),
                     pl.ds(pl.multiple_of(c * width, width), width)],
            prior.at[c], prior_sem.at[c],
        )

    for c in range(chunks):
        load(c).start()

    barrier = pltpu.get_barrier_semaphore()
    for other in range(1, chips):
        pl.semaphore_signal(
            barrier, inc=1, device_id=(mine, lax.rem(chip + other, chips) * 2 + core),
            device_id_type=MESH,
        )
    pl.semaphore_signal(barrier, inc=1, device_id=partner, device_id_type=MESH)
    for step in range(1, groups):
        pl.semaphore_signal(barrier, inc=1, device_id=peer(step), device_id_type=MESH)
    pl.semaphore_wait(barrier, chips + groups - 1)

    def meta_to(other):
        target = lax.rem(chip + other, chips)
        return remote(
            metas.at[place], metas.at[place], meta_send.at[other], meta_recv.at[other],
            (mine, target * 2 + core),
        )

    def meta_partner(q):
        block = metas.at[q * 2 + core]
        return remote(block, block, metap_send.at[q], metap_recv.at[q], partner)

    def to_right(c, q):
        block = rows.at[c, q * 2 + core]
        return remote(block, block, send_r.at[c, chip - q], recv_r.at[c, chip - q], right)

    def to_left(c, q):
        block = rows.at[c, q * 2 + core]
        return remote(block, block, send_l.at[c, q - chip], recv_l.at[c, q - chip], left)

    def to_partner(c, q):
        block = rows.at[c, q * 2 + core]
        return remote(block, block, send_p.at[c, q], recv_p.at[c, q], partner)

    def from_left(c, q):
        block = rows.at[c, q * 2 + core]
        return remote(
            block, block, send_r.at[c, chip - 1 - q], recv_r.at[c, chip - 1 - q], right
        )

    def from_right(c, q):
        block = rows.at[c, q * 2 + core]
        return remote(
            block, block, send_l.at[c, q - chip - 1], recv_l.at[c, q - chip - 1], left
        )

    def from_partner(c, q):
        block = rows.at[c, q * 2 + 1 - core]
        return remote(block, block, send_p.at[c, q], recv_p.at[c, q], partner)

    def issue_own(c):
        @pl.when(chip < chips - 1)
        def _():
            to_right(c, chip).start()

        @pl.when(chip > 0)
        def _():
            to_left(c, chip).start()

        to_partner(c, chip).start()

    load(0).wait()
    issue_own(0)
    for c in range(chunks):
        load_prior(c).start()
    for c in range(1, chunks):
        load(c).wait()

    ids_s = lax.broadcasted_iota(jnp.int32, (shards, block_rows), 0).astype(jnp.float32)
    before = (
        lax.broadcasted_iota(jnp.int32, (block_rows, block_rows), 0)
        < lax.broadcasted_iota(jnp.int32, (block_rows, block_rows), 1)
    ).astype(jnp.bfloat16)
    labels = [[label_in[b, t : t + 1, :].astype(jnp.float32) for t in range(iters)] for b in range(local)]
    ranges = [[jnp.floor((x + 0.5) * (1.0 / owned)) for x in xs] for xs in labels]
    hots = [[(ids_s == x).astype(jnp.float32) for x in xs] for xs in ranges]
    flat = [x for xs in hots for x in xs]
    earlier = jnp.dot(
        jnp.concatenate(flat, axis=0).astype(jnp.bfloat16), before,
        preferred_element_type=jnp.float32,
    )
    lines[...] = jnp.zeros_like(lines)
    for b in range(local):
        total = jnp.zeros((block_rows, width), jnp.float32)
        top = jnp.zeros((block_rows, width), jnp.float32)
        for c in range(chunks):
            x = rows[c, place, b].astype(jnp.float32)
            total = total + x * x
            top = jnp.maximum(top, jnp.abs(x))
        square = jnp.sum(total.T, axis=0, keepdims=True)
        high = square.astype(jnp.bfloat16).astype(jnp.float32)
        middle = (square - high).astype(jnp.bfloat16).astype(jnp.float32)
        lines[0:1, :] = jnp.ones_like(square)
        lines[1:2, :] = high
        lines[2:3, :] = middle
        lines[3:4, :] = square - high - middle
        lines[4:5, :] = jnp.max(top.T, axis=0, keepdims=True)
        lines[5:6, :] = jnp.full((1, block_rows), owner_in[b], jnp.int32).astype(jnp.float32)
        for t in range(iters):
            base = FIXED + 4 * t
            inside = labels[b][t] - ranges[b][t] * owned
            coarse = jnp.floor((inside + 0.5) * (1.0 / 256))
            at = (b * iters + t) * shards
            lines[base : base + 1, :] = inside - 256.0 * coarse
            lines[base + 1 : base + 2, :] = coarse
            lines[base + 2 : base + 3, :] = ranges[b][t]
            lines[base + 3 : base + 4, :] = jnp.sum(
                hots[b][t] * earlier[at : at + shards, :], axis=0, keepdims=True
            )
        metas[place, b] = lines[...].astype(jnp.bfloat16)

    for other in range(1, chips):
        meta_to(other).start()
    issue_own(1)

    on_left, on_right = chip, chips - 1 - chip
    both = jnp.minimum(on_left, on_right)

    def source(k):
        paired = k <= 2 * both
        distance = jnp.where(paired, (k + 1) // 2, k - both)
        is_left = jnp.where(paired, (k % 2) == 1, on_left > on_right)
        return jnp.where(is_left, chip - distance, chip + distance)

    def pull(j):
        c, k = j // chips, j % chips
        q = source(k)

        @pl.when((k == 0) & (c + 2 < chunks))
        def _():
            issue_own(c + 2)

        @pl.when(q < chip)
        def _():
            from_left(c, q).wait_recv()

            @pl.when(chip < chips - 1)
            def _():
                to_right(c, q).start()

            to_partner(c, q).start()

        @pl.when(q > chip)
        def _():
            from_right(c, q).wait_recv()

            @pl.when(chip > 0)
            def _():
                to_left(c, q).start()

            to_partner(c, q).start()

    ids_r = lax.broadcasted_iota(jnp.int32, (slots, block_rows), 0)
    ids_c = lax.broadcasted_iota(jnp.int32, (owned, slots), 0)

    ext[...] = jnp.zeros_like(ext)
    acc[...] = jnp.zeros_like(acc)

    def take_meta(q, core_of):
        origin = q * 2 + core_of
        for t in range(iters):
            base = FIXED + 4 * t
            wide = jnp.zeros((META_ROWS, slots), jnp.float32)
            for b in range(local):
                e = metas[origin, b]
                f = e.astype(jnp.float32)
                wanted = f[base + 2 : base + 3, :].astype(jnp.int32) == place
                pos = jnp.where(wanted, f[base + 3 : base + 4, :].astype(jnp.int32) + b * most, -1)
                hot = (ids_r == pos).astype(jnp.bfloat16)
                select[origin, b, t * most : (t + 1) * most, :] = hot[b * most : (b + 1) * most, :]
                wide = wide + lax.dot_general(
                    e, hot, (((1,), (1,)), ((), ())), preferred_element_type=jnp.float32
                )
            step = wide[5:6, :].astype(jnp.int32) - mine
            step = jnp.where(step < 0, step + groups, step)
            label = wide[base : base + 1, :] + 256.0 * wide[base + 1 : base + 2, :]
            cell = jnp.where(wide[0:1, :] > 0.5, step * owned + label.astype(jnp.int32), -1)
            packed = wide.astype(jnp.bfloat16)
            for g in range(groups):
                hot = (ids_c == cell - g * owned).astype(jnp.bfloat16)
                place_in[t, q, g * owned : (g + 1) * owned, core_of * slots : (core_of + 1) * slots] = hot
                ext[g, t] += lax.dot_general(
                    packed, hot, (((1,), (1,)), ((), ())), preferred_element_type=jnp.float32
                )

    def meta_step(k, carry):
        q = source(k)

        @pl.when(q != chip)
        def _():
            other = lax.rem(chip - q + chips, chips)
            block = metas.at[q * 2 + core]
            remote(block, block, meta_send.at[other], meta_recv.at[other], left).wait_recv()

        meta_partner(q).start()
        for core_of in range(2):

            @pl.when(core_of != core)
            def _():
                block = metas.at[q * 2 + 1 - core]
                remote(block, block, metap_send.at[q], metap_recv.at[q], partner).wait_recv()

        for core_of in range(2):
            take_meta(q, core_of)
        pull(k)
        return carry

    lax.fori_loop(0, chips, meta_step, 0)

    def ext_to(step):
        return remote(
            ext.at[step], ext_recv.at[step - 1], ext_ssem.at[step - 1], ext_rsem.at[step - 1],
            peer(step),
        )

    for step in range(1, groups):
        ext_to(step).start()

    def tall(row):
        return jnp.broadcast_to(row, (LANES, LANES)).T

    for step in range(1, groups):
        for t in range(iters):
            for i in range(reps):
                bound = ext[step, t, 4:5, i * LANES : (i + 1) * LANES]
                inv[step - 1, t, i * LANES : (i + 1) * LANES, :] = tall(
                    LEVELS / jnp.maximum(bound, 1e-30)
                )

    def swap(c, step):
        return remote(
            send.at[c, step - 1], recv.at[c, step - 1], swap_send.at[c, step - 1],
            swap_recv.at[c, step - 1], peer(step),
        )

    tile = owned

    def tally(c, q, first):
        for core_of in range(2):
            origin = q * 2 + core_of
            for b in range(local):
                got = jnp.dot(
                    select[origin, b], rows[c, origin, b], preferred_element_type=jnp.float32
                ).astype(jnp.bfloat16)
                for t in range(iters):
                    compact[t, core_of * slots + b * most : core_of * slots + (b + 1) * most, :] = got[
                        t * most : (t + 1) * most, :
                    ]

        def body(i, carry):
            for t in range(iters):
                part = pl.ds(pl.multiple_of(i * tile, tile), tile)
                acc[t, part, :] += jnp.dot(
                    place_in[t, q, part, :], compact[t], preferred_element_type=jnp.float32
                )
            return carry

        lax.fori_loop(0, groups, body, 0)

    def settle(c):
        for t in range(iters):
            own[c, t] = acc[t, :owned, :]
        for step in range(1, groups):
            part = slice(step * owned, (step + 1) * owned)
            high = (acc[0, part, :] * inv[step - 1, 0] + (HALF + 0.5)).astype(jnp.int32)
            low = (acc[1, part, :] * inv[step - 1, 1] + (HALF + 0.5)).astype(jnp.int32)
            send[c, step - 1] = (high << 16) | low
            swap(c, step).start()
        acc[...] = jnp.zeros_like(acc)

    def scales():
        for step in range(1, groups):
            ext_to(step).wait_recv()
        for t in range(iters):
            for i in range(reps):
                part = slice(i * LANES, (i + 1) * LANES)
                count = ext[0, t, 0:1, part]
                for step in range(1, groups):
                    count = count + ext_recv[step - 1, t, 0:1, part]
                    scale[step - 1, t, part, :] = tall(ext_recv[step - 1, t, 4:5, part] / LEVELS)
                cnt[t, part, :] = tall(count)
        within[...] = jnp.zeros_like(within)

    def finish(c):
        load_prior(c).wait()
        for step in range(1, groups):
            swap(c, step).wait_recv()
        for i in range(reps):
            part = slice(i * LANES, (i + 1) * LANES)
            sums = [own[c, t, part, :] for t in range(iters)]
            for step in range(1, groups):
                word = recv[c, step - 1, part, :]
                high = lax.shift_right_logical(word, 16)
                low = word & 0xFFFF
                for t, code in enumerate((high, low)):
                    sums[t] = sums[t] + (code.astype(jnp.float32) - HALF) * scale[step - 1, t, part, :]
            previous = prior[c, part, :]
            for t in range(iters):
                count = cnt[t, part, :]
                if t == iters - 1:
                    within[part, :] += previous * (count * previous - 2.0 * sums[t])
                previous = (sums[t] + PRIOR * previous) / (count + PRIOR)
            out[part, pl.ds(pl.multiple_of(c * width, width), width)] = previous

    def main_step(j, carry):
        c, k = j // chips, j % chips
        q = source(k)
        ahead = j + jnp.where(both > 0, chips, 0)

        @pl.when((ahead >= chips) & (ahead < chunks * chips))
        def _():
            pull(ahead)

        from_partner(c, q).wait_recv()
        tally(c, q, k == 0)

        @pl.when(k == chips - 1)
        def _():
            settle(c)

            @pl.when(c == 0)
            def _():
                scales()

            @pl.when(c > 0)
            def _():
                finish(c - 1)

        return carry

    lax.fori_loop(0, chunks * chips, main_step, 0)
    finish(chunks - 1)

    for i in range(reps):
        part = slice(i * LANES, (i + 1) * LANES)
        spread = jnp.sum(within[part, :].T, axis=0, keepdims=True)
        last = iters - 1
        count = ext[0, last, 0:1, part]
        square = ext[0, last, 1:2, part] + ext[0, last, 2:3, part] + ext[0, last, 3:4, part]
        for step in range(1, groups):
            far = ext_recv[step - 1, last, :, part]
            count = count + far[0:1]
            square = square + far[1:2] + far[2:3] + far[3:4]
        inertia[:, part] = (spread + square) / ((count + PRIOR) * features)

    for other in range(1, chips):
        meta_to(other).wait_send()
    for q in range(chips):
        meta_partner(q).wait_send()
    for step in range(1, groups):
        ext_to(step).wait_send()

    def drain(j, carry):
        c, q = j // chips, j % chips

        @pl.when((q <= chip) & (chip < chips - 1))
        def _():
            to_right(c, q).wait_send()

        @pl.when((q >= chip) & (chip > 0))
        def _():
            to_left(c, q).wait_send()

        to_partner(c, q).wait_send()
        return carry

    lax.fori_loop(0, chunks * chips, drain, 0)
    for c in range(chunks):
        for step in range(1, groups):
            swap(c, step).wait_send()


def fused_buffers(local, block_rows, features, iters, owned, groups, shards):
    chips = shards // 2
    most = 2 * block_rows // shards
    width, chunks = LANES, features // LANES
    slots = local * most
    vmem = pltpu.VMEM
    f32, b16, i32 = jnp.float32, jnp.bfloat16, jnp.int32
    buffers = [
        ((chunks, shards, local, block_rows, width), b16),
        ((shards, local, META_ROWS, block_rows), b16),
        ((shards, local, iters * most, block_rows), b16),
        ((iters, chips, groups * owned, 2 * slots), b16),
        ((iters, groups * owned, width), f32),
        ((iters, 2 * slots, width), b16),
        ((chunks, iters, owned, width), f32),
        ((chunks, groups - 1, owned, width), i32),
        ((chunks, groups - 1, owned, width), i32),
        ((groups - 1, iters, owned, width), f32),
        ((groups - 1, iters, owned, width), f32),
        ((iters, owned, width), f32),
        ((groups, iters, META_ROWS, owned), f32),
        ((groups - 1, iters, META_ROWS, owned), f32),
        ((chunks, owned, width), f32),
        ((owned, width), f32),
        ((META_ROWS, block_rows), f32),
    ]
    dma = pltpu.SemaphoreType.DMA
    sems = [dma((chunks,)), dma((chunks,))]
    sems += [dma((chips,))] * 4
    sems += [dma((chunks, chips))] * 6
    sems += [dma((groups - 1,))] * 2
    sems += [dma((chunks, groups - 1))] * 2
    return [vmem(s, d) for s, d in buffers], sems, buffers, most, chunks


def fits(local, block_rows, features, iters, owned, groups, shards):
    if features % LANES or features < 2 * LANES or owned % LANES or shards % 2:
        return False
    if iters != 2 or 4 * iters + FIXED > META_ROWS or (2 * block_rows) % shards:
        return False
    most = 2 * block_rows // shards
    if (local * most) % LANES or most % 16 or block_rows % LANES:
        return False
    total = 0
    for shape, dtype in fused_buffers(local, block_rows, features, iters, owned, groups, shards)[2]:
        size = jnp.dtype(dtype).itemsize
        for extent in shape:
            size *= extent
        total += size
    return total < 58 * 2**20


def fused_body(embeddings, assignments, block_group, centroids):
    groups, shards = lax.axis_size("group"), lax.axis_size("shard")
    local, block_rows, features = embeddings.shape
    iters = assignments.shape[1]
    owned = centroids.shape[1] // shards
    buffers, sems, unused, most, chunks = fused_buffers(
        local, block_rows, features, iters, owned, groups, shards
    )

    out, inertia = pl.pallas_call(
        functools.partial(fused_kernel, chunks, most),
        out_shape=[
            pltpu.VMEM((owned, features), jnp.float32),
            pltpu.VMEM((1, owned), jnp.float32),
        ],
        in_specs=[
            pl.BlockSpec(memory_space=pltpu.SMEM),
            pl.BlockSpec(memory_space=pltpu.VMEM),
            pl.BlockSpec(memory_space=pl.ANY),
            pl.BlockSpec(memory_space=pl.ANY),
        ],
        out_specs=[pl.BlockSpec(memory_space=pltpu.VMEM)] * 2,
        scratch_shapes=buffers + sems,
        compiler_params=pltpu.CompilerParams(
            collective_id=0, has_side_effects=True, vmem_limit_bytes=56 * 2**20
        ),
    )(block_group, assignments, embeddings, centroids)
    return out[None], inertia


def choose(embeddings, assignments, block_group, centroids):
    groups, shards = lax.axis_size("group"), lax.axis_size("shard")
    local, block_rows, features = embeddings.shape
    owned = centroids.shape[1] // shards
    if fits(local, block_rows, features, assignments.shape[1], owned, groups, shards):
        return fused_body(embeddings, assignments, block_group, centroids)
    return body(embeddings, assignments, block_group, centroids)


def solution(mesh):
    in_specs = (
        P(("group", "shard"), None, None),
        P(("group", "shard"), None, None),
        P(("group", "shard")),
        P("group", None, None),
    )
    out_specs = (P("group", "shard", None), P("group", "shard"))
    return jax.shard_map(choose, mesh=mesh, in_specs=in_specs, out_specs=out_specs, check_vma=False)
```

```python
import functools

import jax
import jax.numpy as jnp
from jax import lax
from jax.experimental import pallas as pl
from jax.experimental.pallas import tpu as pltpu
from jax.sharding import PartitionSpec as P

PRIOR = 8.0
META = 8
CHUNKS = 3
MESH = pl.DeviceIdType.MESH


def exchange_kernel(n_gather, n_swap, width, column, *refs):
    n_in = n_gather + n_swap
    gathers, swaps = refs[:n_gather], refs[n_gather:n_in]
    outs = refs[n_in : 2 * n_in]
    gather_outs, swap_outs = outs[:n_gather], outs[n_gather:]
    scratch = refs[2 * n_in :]
    stages = scratch[:n_gather]
    scratch = scratch[n_gather:]

    groups, shards = lax.axis_size("group"), lax.axis_size("shard")
    chips = shards // 2
    mine, place = lax.axis_index("group"), lax.axis_index("shard")
    chip, core = place // 2, place % 2
    partner = (mine, chip * 2 + 1 - core)
    right = (mine, lax.rem(chip + 1, chips) * 2 + core)
    left = (mine, lax.rem(chip + chips - 1, chips) * 2 + core)

    def peer(step):
        return lax.rem(mine + step, groups)

    barrier = pltpu.get_barrier_semaphore()
    greeted = 0
    if n_gather:
        for device in (left, right, partner):
            pl.semaphore_signal(barrier, inc=1, device_id=device, device_id_type=MESH)
        greeted += 3
    if n_swap:
        for step in range(1, groups):
            pl.semaphore_signal(
                barrier, inc=1, device_id=(peer(step), place), device_id_type=MESH
            )
        greeted += groups - 1

    loads = []
    if n_gather:
        load_sem = scratch[0]
        for i in range(n_gather):
            source = gathers[i]
            if i == 0:
                source = source.at[:, :, pl.ds(column, width)]
            load = pltpu.make_async_copy(source, stages[i], load_sem.at[i])
            load.start()
            loads.append(load)
    pl.semaphore_wait(barrier, greeted)

    swap_copies = []
    if n_swap:
        swap_send, swap_recv = scratch[-2:]
        for step in range(1, groups):
            for i in range(n_swap):
                copy = pltpu.make_async_remote_copy(
                    src_ref=swaps[i].at[peer(step)],
                    dst_ref=swap_outs[i].at[step - 1],
                    send_sem=swap_send.at[i, step - 1],
                    recv_sem=swap_recv.at[i, step - 1],
                    device_id=(peer(step), place),
                    device_id_type=MESH,
                )
                copy.start()
                swap_copies.append(copy)

    if n_gather:
        store_sem, send_r, recv_r, send_l, recv_l, send_p, recv_p = scratch[1:8]
        stores = []

        def hop(i, source, origin, step, to, sends, recvs):
            return pltpu.make_async_remote_copy(
                src_ref=source,
                dst_ref=gather_outs[i].at[origin * 2 + core],
                send_sem=sends.at[i, step],
                recv_sem=recvs.at[i, step],
                device_id=to,
                device_id_type=MESH,
            )

        for i in range(n_gather):
            loads[i].wait()
            store = pltpu.make_async_copy(
                stages[i], gather_outs[i].at[place], store_sem.at[i]
            )

            @pl.when(chip < chips - 1)
            def _():
                hop(i, stages[i], chip, 0, right, send_r, recv_r).start()

            @pl.when(chip > 0)
            def _():
                hop(i, stages[i], chip, 0, left, send_l, recv_l).start()

            hop(i, stages[i], chip, chip, partner, send_p, recv_p).start()
            store.start()
            stores.append(store)

        for step in range(chips - 1):
            for i in range(n_gather):
                from_left = chip - 1 - step

                @pl.when(from_left >= 0)
                def _():
                    block = gather_outs[i].at[from_left * 2 + core]
                    hop(i, block, from_left, step, right, send_r, recv_r).wait_recv()

                    if step < chips - 2:

                        @pl.when(chip < chips - 1)
                        def _():
                            hop(i, block, from_left, step + 1, right, send_r, recv_r).start()

                    hop(i, block, from_left, from_left, partner, send_p, recv_p).start()

                from_right = chip + 1 + step

                @pl.when(from_right <= chips - 1)
                def _():
                    block = gather_outs[i].at[from_right * 2 + core]
                    hop(i, block, from_right, step, left, send_l, recv_l).wait_recv()

                    if step < chips - 2:

                        @pl.when(chip > 0)
                        def _():
                            hop(i, block, from_right, step + 1, left, send_l, recv_l).start()

                    hop(i, block, from_right, from_right, partner, send_p, recv_p).start()

        for i in range(n_gather):
            stores[i].wait()
            for step in range(chips - 1):

                @pl.when((chip - step >= 0) & (chip < chips - 1))
                def _():
                    hop(i, stages[i], chip, step, right, send_r, recv_r).wait_send()

                @pl.when((chip + step <= chips - 1) & (chip > 0))
                def _():
                    hop(i, stages[i], chip, step, left, send_l, recv_l).wait_send()

            for origin in range(chips):
                hop(i, stages[i], origin, origin, partner, send_p, recv_p).wait()

    for copy in swap_copies:
        copy.wait()


def exchange(gathers, swaps, width, column, key):
    groups, shards = lax.axis_size("group"), lax.axis_size("shard")
    chips = shards // 2
    n_gather, n_swap = len(gathers), len(swaps)
    shapes, scratch = [], []
    for i, array in enumerate(gathers):
        block = array.shape[:-1] + (width if i == 0 else array.shape[-1],)
        shapes.append(jax.ShapeDtypeStruct((shards,) + block, array.dtype))
        scratch.append(pltpu.VMEM(block, array.dtype))
    for array in swaps:
        shapes.append(jax.ShapeDtypeStruct((groups - 1,) + array.shape[1:], array.dtype))
    dma = pltpu.SemaphoreType.DMA
    if n_gather:
        scratch += [dma((n_gather,)), dma((n_gather,))]
        scratch += [dma((n_gather, max(chips - 1, 1)))] * 4
        scratch += [dma((n_gather, chips))] * 2
    if n_swap:
        scratch += [dma((n_swap, groups - 1))] * 2
    return pl.pallas_call(
        functools.partial(exchange_kernel, n_gather, n_swap, width, column),
        out_shape=shapes,
        in_specs=[pl.BlockSpec(memory_space=pl.ANY)] * (n_gather + n_swap),
        out_specs=[pl.BlockSpec(memory_space=pl.ANY)] * (n_gather + n_swap),
        scratch_shapes=scratch,
        compiler_params=pltpu.CompilerParams(collective_id=key, has_side_effects=True),
    )(*gathers, *swaps)


def tally_kernel(per_step, iters, with_extra, owners, labels, extra, rows, sums, *more):
    step = pl.program_id(0)
    centers = sums.shape[2]
    block_rows = rows.shape[1]

    @pl.when(step == 0)
    def _():
        sums[...] = jnp.zeros_like(sums)
        if with_extra:
            more[0][...] = jnp.zeros_like(more[0])

    ids = lax.broadcasted_iota(jnp.int32, (centers, block_rows), 0)
    for block in range(per_step):
        owner = owners[step * per_step + block]
        for t in range(iters):
            onehot = (ids == labels[block, t : t + 1, :]).astype(jnp.bfloat16)
            sums[owner, t] += jnp.dot(
                onehot, rows[block], preferred_element_type=jnp.float32
            )
            if with_extra:
                more[0][owner, t] += lax.dot_general(
                    extra[block],
                    onehot,
                    (((1,), (1,)), ((), ())),
                    preferred_element_type=jnp.float32,
                )


def tally(owners, labels, extra, rows, groups, centers, per_step, with_extra):
    blocks, iters, block_rows = labels.shape
    width = rows.shape[-1]
    shapes = [jax.ShapeDtypeStruct((groups, iters, centers, width), jnp.float32)]
    if with_extra:
        shapes.append(jax.ShapeDtypeStruct((groups, iters, extra.shape[1], centers), jnp.float32))
    out_specs = [pl.BlockSpec(s.shape, lambda i, o: (0, 0, 0, 0)) for s in shapes]
    return pl.pallas_call(
        functools.partial(tally_kernel, per_step, iters, with_extra),
        out_shape=shapes,
        grid_spec=pltpu.PrefetchScalarGridSpec(
            num_scalar_prefetch=1,
            grid=(blocks // per_step,),
            in_specs=[
                pl.BlockSpec((per_step, iters, block_rows), lambda i, o: (i, 0, 0)),
                pl.BlockSpec((per_step,) + extra.shape[1:], lambda i, o: (i, 0, 0)),
                pl.BlockSpec((per_step, block_rows, width), lambda i, o: (i, 0, 0)),
            ],
            out_specs=out_specs,
        ),
        compiler_params=pltpu.CompilerParams(vmem_limit_bytes=48 * 2**20),
    )(owners, labels, extra, rows)


def body(embeddings, assignments, block_group, centroids):
    groups, shards = lax.axis_size("group"), lax.axis_size("shard")
    mine, place = lax.axis_index("group"), lax.axis_index("shard")
    local, block_rows, features = embeddings.shape
    iters = assignments.shape[1]
    owned = centroids.shape[1] // shards
    chunks = CHUNKS if features % (CHUNKS * 128) == 0 else 1
    width = features // chunks
    blocks = shards * local

    wide = embeddings.astype(jnp.float32)
    squares = jnp.sum(wide * wide, axis=2)
    meta = jnp.concatenate(
        [
            assignments.astype(jnp.float32),
            jnp.broadcast_to(
                block_group[:, None, None].astype(jnp.float32), (local, 1, block_rows)
            ),
            squares[:, None, :],
            jnp.zeros((local, META - iters - 2, block_rows), jnp.float32),
        ],
        axis=1,
    )

    rows, metas = exchange([embeddings, meta], [], width, 0, 0)
    metas = metas.reshape(blocks, META, block_rows)
    labels = metas[:, :iters].astype(jnp.int32) - place * owned
    owners = metas[:, iters, 0].astype(jnp.int32)
    square = metas[:, iters + 1]
    high = lax.reduce_precision(square, 8, 7)
    middle = lax.reduce_precision(square - high, 8, 7)
    low = square - high - middle
    one = jnp.ones_like(square)
    zero = jnp.zeros_like(square)
    extra = jnp.stack([one, high, middle, low] + [zero] * 12, axis=1).astype(jnp.bfloat16)

    totals = []
    tail = None
    pending = []
    for chunk in range(chunks):
        result = tally(
            owners,
            labels,
            extra,
            rows.reshape(blocks, block_rows, width),
            groups,
            owned,
            local,
            chunk == 0,
        )
        column = (chunk + 1) * width
        if chunk + 1 < chunks:
            rows, *got = exchange([embeddings], result, width, column, chunk + 1)
        else:
            got = exchange([], result, width, 0, chunk + 1)
        whole = [
            lax.dynamic_index_in_dim(kept, mine, 0, keepdims=False) + jnp.sum(came, axis=0)
            for kept, came in zip(result, got)
        ]
        totals.append(whole[0])
        if chunk == 0:
            tail = whole[1]

    prior = lax.dynamic_slice_in_dim(centroids[0], place * owned, owned, 0)
    counts = tail[:, 0]
    within = tail[iters - 1, 1] + tail[iters - 1, 2] + tail[iters - 1, 3]
    pieces = []
    for chunk in range(chunks):
        previous = prior[:, chunk * width : (chunk + 1) * width]
        for t in range(iters):
            sums = totals[chunk][t]
            count = counts[t][:, None]
            if t == iters - 1:
                within = within + jnp.sum(
                    previous * (count * previous - 2.0 * sums), axis=1
                )
            previous = (sums + PRIOR * previous) / (count + PRIOR)
        pieces.append(previous)
    inertia = within / ((counts[iters - 1] + PRIOR) * features)
    return (jnp.concatenate(pieces, axis=1)[None], inertia[None])


LANES = 128
META_ROWS = 16
FIXED = 6
CAP = 2
LEVELS = 32000.0
HALF = 32768.0


def fused_kernel(
    chunks, late, most, owner_in, label_in, emb, cents, out, inertia,
    rows, metas, select, place_in, acc, compact, own, send, recv, inv, scale, cnt, ext,
    ext_recv, prior, within, lines, share,
    late_own, late_send, late_rows, late_meta_send, late_metas, late_select, late_cells, late_compact,
    late_acc, late_out, late_in, late_scale_out, late_scale_in,
    load_sem, prior_sem, meta_send, meta_recv, metap_send, metap_recv,
    send_r, recv_r, send_l, recv_l, send_p, recv_p, ext_ssem, ext_rsem, swap_send, swap_recv,
    late_load_sem, lswap_s, lswap_r, lpart_s, lpart_r, lin_s, lin_r, lshare_s, lshare_r,
    code_s, code_r, scale_s, scale_r,
):
    groups, shards = lax.axis_size("group"), lax.axis_size("shard")
    chips = shards // 2
    mine, place = lax.axis_index("group"), lax.axis_index("shard")
    chip, core = place // 2, place % 2
    partner = (mine, chip * 2 + 1 - core)
    right, left = (mine, place + 2), (mine, place - 2)
    is_end = (chip == 0) | (chip == chips - 1)
    mate = chip + 1 - 2 * lax.rem(chip, 2)
    targets = [place, (chips - 1 - chip) * 2 + core, (chips - 1 - mate) * 2 + core, mate * 2 + core]
    local, block_rows, features = emb.shape
    width = rows.shape[-1]
    iters = place_in.shape[0]
    owned = own.shape[2]
    slots = CAP * most
    reps = owned // LANES

    def peer(step):
        return (lax.rem(mine + step, groups), place)

    def remote(src, dst, ssem, rsem, to):
        return pltpu.make_async_remote_copy(
            src_ref=src, dst_ref=dst, send_sem=ssem, recv_sem=rsem,
            device_id=to, device_id_type=MESH,
        )

    def load(c):
        return pltpu.make_async_copy(
            emb.at[:, :, pl.ds(pl.multiple_of(c * width, width), width)],
            rows.at[c, place], load_sem.at[c],
        )

    def load_late(x):
        at = (chunks + x) * width
        return pltpu.make_async_copy(
            emb.at[:, :, pl.ds(at, width)], late_own.at[x], late_load_sem.at[x]
        )

    def load_prior(c):
        return pltpu.make_async_copy(
            cents.at[0, pl.ds(pl.multiple_of(place * owned, owned), owned),
                     pl.ds(pl.multiple_of(c * width, width), width)],
            prior.at[c], prior_sem.at[c],
        )

    for c in range(chunks):
        load(c).start()
    for x in range(late):
        load_late(x).start()

    barrier = pltpu.get_barrier_semaphore()
    for other in range(1, chips):
        pl.semaphore_signal(
            barrier, inc=1, device_id=(mine, lax.rem(chip + other, chips) * 2 + core),
            device_id_type=MESH,
        )
    pl.semaphore_signal(barrier, inc=1, device_id=partner, device_id_type=MESH)
    for step in range(1, groups):
        pl.semaphore_signal(barrier, inc=1, device_id=peer(step), device_id_type=MESH)
    pl.semaphore_wait(barrier, chips + groups - 1)

    def meta_to(other):
        target = lax.rem(chip + other, chips)
        return remote(
            metas.at[place], metas.at[place], meta_send.at[other], meta_recv.at[other],
            (mine, target * 2 + core),
        )

    def meta_partner(q):
        block = metas.at[q * 2 + core]
        return remote(block, block, metap_send.at[q], metap_recv.at[q], partner)

    def to_right(c, q):
        block = rows.at[c, q * 2 + core]
        return remote(block, block, send_r.at[c, chip - q], recv_r.at[c, chip - q], right)

    def to_left(c, q):
        block = rows.at[c, q * 2 + core]
        return remote(block, block, send_l.at[c, q - chip], recv_l.at[c, q - chip], left)

    def to_partner(c, q):
        block = rows.at[c, q * 2 + core]
        return remote(block, block, send_p.at[c, q], recv_p.at[c, q], partner)

    def from_left(c, q):
        block = rows.at[c, q * 2 + core]
        return remote(
            block, block, send_r.at[c, chip - 1 - q], recv_r.at[c, chip - 1 - q], right
        )

    def from_right(c, q):
        block = rows.at[c, q * 2 + core]
        return remote(
            block, block, send_l.at[c, q - chip - 1], recv_l.at[c, q - chip - 1], left
        )

    def from_partner(c, q):
        block = rows.at[c, q * 2 + 1 - core]
        return remote(block, block, send_p.at[c, q], recv_p.at[c, q], partner)

    def issue_own(c):
        @pl.when(chip < chips - 1)
        def _():
            to_right(c, chip).start()

        @pl.when(chip > 0)
        def _():
            to_left(c, chip).start()

        to_partner(c, chip).start()

    load(0).wait()
    load(1).wait()
    issue_own(0)
    for c in range(chunks + late):
        load_prior(c).start()
    for c in range(2, chunks):
        load(c).wait()
    for x in range(late):
        load_late(x).wait()

    ids_s = lax.broadcasted_iota(jnp.int32, (shards, block_rows), 0).astype(jnp.float32)
    before = (
        lax.broadcasted_iota(jnp.int32, (block_rows, block_rows), 0)
        < lax.broadcasted_iota(jnp.int32, (block_rows, block_rows), 1)
    ).astype(jnp.bfloat16)
    labels = [[label_in[b, t : t + 1, :].astype(jnp.float32) for t in range(iters)] for b in range(local)]
    ranges = [[jnp.floor((x + 0.5) * (1.0 / owned)) for x in xs] for xs in labels]
    hots = [[(ids_s == x).astype(jnp.float32) for x in xs] for xs in ranges]
    flat = [x for xs in hots for x in xs]
    earlier = jnp.dot(
        jnp.concatenate(flat, axis=0).astype(jnp.bfloat16), before,
        preferred_element_type=jnp.float32,
    )
    lines[...] = jnp.zeros_like(lines)
    for b in range(local):
        total = jnp.zeros((block_rows, width), jnp.float32)
        top = jnp.zeros((block_rows, width), jnp.float32)
        for c in range(chunks + late):
            x = rows[c, place, b] if c < chunks else late_own[c - chunks, b]
            x = x.astype(jnp.float32)
            total = total + x * x
            top = jnp.maximum(top, jnp.abs(x))
        square = jnp.sum(total.T, axis=0, keepdims=True)
        high = square.astype(jnp.bfloat16).astype(jnp.float32)
        middle = (square - high).astype(jnp.bfloat16).astype(jnp.float32)
        lines[0:1, :] = jnp.ones_like(square)
        lines[1:2, :] = high
        lines[2:3, :] = middle
        lines[3:4, :] = square - high - middle
        lines[4:5, :] = jnp.max(top.T, axis=0, keepdims=True)
        turn = owner_in[b] * CAP
        for other in range(b):
            turn = turn + jnp.where(owner_in[other] == owner_in[b], 1, 0)
        lines[5:6, :] = jnp.full((1, block_rows), turn, jnp.int32).astype(jnp.float32)
        for t in range(iters):
            base = FIXED + 4 * t
            inside = labels[b][t] - ranges[b][t] * owned
            coarse = jnp.floor((inside + 0.5) * (1.0 / 256))
            at = (b * iters + t) * shards
            lines[base : base + 1, :] = inside - 256.0 * coarse
            lines[base + 1 : base + 2, :] = coarse
            lines[base + 2 : base + 3, :] = ranges[b][t]
            lines[base + 3 : base + 4, :] = jnp.sum(
                hots[b][t] * earlier[at : at + shards, :], axis=0, keepdims=True
            )
        metas[place, b] = lines[...].astype(jnp.bfloat16)

    for other in range(1, chips):
        meta_to(other).start()
    issue_own(1)

    def late_swap(x, step):
        sent = late_meta_send if x == late else late_send.at[x]
        kept = late_metas if x == late else late_rows.at[x]
        return remote(
            sent.at[step - 1], kept.at[core, step], lswap_s.at[x, step - 1],
            lswap_r.at[x, step - 1], peer(step),
        )

    def late_block(x, at):
        return late_metas.at[at] if x == late else late_rows.at[x, at]

    def late_partner(x):
        block = late_block(x, core)
        return remote(block, block, lpart_s.at[x], lpart_r.at[x], partner)

    def late_inward(x):
        return remote(
            late_block(x, core), late_block(x, 2 + core), lin_s.at[x], lin_r.at[x],
            (mine, mate * 2 + core),
        )

    def late_share(x):
        block = late_block(x, 2 + core)
        return remote(block, block, lshare_s.at[x], lshare_r.at[x], partner)

    def late_start():
        for x in (late,) + tuple(range(late)):
            for step in range(1, groups):
                late_swap(x, step).wait_recv()
            late_partner(x).start()

            @pl.when(is_end)
            def _():
                late_inward(x).start()

    chosen = []
    for b in range(local):
        turn = metas[place, b].astype(jnp.float32)[5:6, :LANES].astype(jnp.int32) - mine * CAP
        chosen.append(jnp.where(turn < 0, turn + groups * CAP, turn))
    for step in range(groups):
        for i in range(CAP):
            weights = [
                jnp.broadcast_to(
                    (turn == step * CAP + i).astype(jnp.float32), (META_ROWS, LANES)
                ).astype(jnp.bfloat16)
                for turn in chosen
            ]

            def pick(blocks):
                tiles = [x.reshape(x.shape[0] // META_ROWS, META_ROWS, LANES) for x in blocks]
                put = tiles[0] * weights[0][None]
                for b in range(1, local):
                    put = put + tiles[b] * weights[b][None]
                return put.reshape(blocks[0].shape)

            for lane in range(0, block_rows, LANES):
                part = slice(lane, lane + LANES)
                put = pick([metas[place, b, :, part] for b in range(local)])
                if step == 0:
                    late_metas[core, 0, i, :, part] = put
                else:
                    late_meta_send[step - 1, i, :, part] = put
            for x in range(late):
                put = pick([late_own[x, b] for b in range(local)])
                if step == 0:
                    late_rows[x, core, 0, i] = put
                else:
                    late_send[x, step - 1, i] = put
    for x in (late,) + tuple(range(late)):
        for step in range(1, groups):
            late_swap(x, step).start()

    on_left, on_right = chip, chips - 1 - chip
    both = jnp.minimum(on_left, on_right)

    def source(k):
        paired = k <= 2 * both
        distance = jnp.where(paired, (k + 1) // 2, k - both)
        is_left = jnp.where(paired, (k % 2) == 1, on_left > on_right)
        return jnp.where(is_left, chip - distance, chip + distance)

    def pull(j):
        c, k = j // chips, j % chips
        q = source(k)

        @pl.when((k == 0) & (c + 2 < chunks))
        def _():
            issue_own(c + 2)

        @pl.when(q < chip)
        def _():
            from_left(c, q).wait_recv()

            @pl.when(chip < chips - 1)
            def _():
                to_right(c, q).start()

            to_partner(c, q).start()

        @pl.when(q > chip)
        def _():
            from_right(c, q).wait_recv()

            @pl.when(chip > 0)
            def _():
                to_left(c, q).start()

            to_partner(c, q).start()

    ids_m = lax.rem(lax.broadcasted_iota(jnp.int32, (slots, block_rows), 0), most)
    ids_c = lax.broadcasted_iota(jnp.int32, (owned, slots), 0)
    turns = lax.broadcasted_iota(jnp.int32, (1, slots), 1) // most

    ext[...] = jnp.zeros_like(ext)
    acc[...] = jnp.zeros_like(acc)
    late_acc[...] = jnp.zeros_like(late_acc)
    late_scale_out[...] = jnp.zeros_like(late_scale_out)

    def take_meta(q, core_of):
        origin = q * 2 + core_of
        rel = []
        for b in range(local):
            place_of = metas[origin, b].astype(jnp.float32)[5:6, :slots].astype(jnp.int32) - mine * CAP
            rel.append(jnp.where(place_of < 0, place_of + groups * CAP, place_of))
            for i in range(groups * CAP):
                one = (rel[b] == i).astype(jnp.float32)[:, :LANES]
                share[origin, b, i] = jnp.broadcast_to(one, (16, LANES)).astype(jnp.bfloat16)
        for t in range(iters):
            base = FIXED + 4 * t
            found = []
            for b in range(local):
                e = metas[origin, b]
                f = e.astype(jnp.float32)
                wanted = f[base + 2 : base + 3, :].astype(jnp.int32) == place
                pos = jnp.where(wanted, f[base + 3 : base + 4, :].astype(jnp.int32), -1)
                hot = (ids_m == pos).astype(jnp.bfloat16)
                select[origin, b, t * most : (t + 1) * most, :] = hot[:most, :]
                found.append(
                    lax.dot_general(
                        e, hot, (((1,), (1,)), ((), ())), preferred_element_type=jnp.float32
                    )
                )
            for g in range(groups):
                pair = jnp.zeros((META_ROWS, slots), jnp.float32)
                for b in range(local):
                    pair = pair + jnp.where(rel[b] == turns + g * CAP, found[b], 0.0)
                label = pair[base : base + 1, :] + 256.0 * pair[base + 1 : base + 2, :]
                cell = jnp.where(pair[0:1, :] > 0.5, label.astype(jnp.int32), -1)
                hot = (ids_c == cell).astype(jnp.bfloat16)
                part = slice(core_of * slots, (core_of + 1) * slots)
                place_in[t, q, g * owned : (g + 1) * owned, part] = hot
                ext[g, t] += lax.dot_general(
                    pair.astype(jnp.bfloat16), hot, (((1,), (1,)), ((), ())),
                    preferred_element_type=jnp.float32,
                )

    def meta_step(k, carry):
        q = source(k)

        @pl.when(q != chip)
        def _():
            other = lax.rem(chip - q + chips, chips)
            block = metas.at[q * 2 + core]
            remote(block, block, meta_send.at[other], meta_recv.at[other], left).wait_recv()

        meta_partner(q).start()
        for core_of in range(2):

            @pl.when(core_of != core)
            def _():
                block = metas.at[q * 2 + 1 - core]
                remote(block, block, metap_send.at[q], metap_recv.at[q], partner).wait_recv()

        for core_of in range(2):
            take_meta(q, core_of)
        pull(k)
        return carry

    lax.fori_loop(0, chips, meta_step, 0)
    late_start()

    def ext_to(step):
        return remote(
            ext.at[step], ext_recv.at[step - 1], ext_ssem.at[step - 1], ext_rsem.at[step - 1],
            peer(step),
        )

    for step in range(1, groups):
        ext_to(step).start()

    def tall(row):
        return jnp.broadcast_to(row, (LANES, LANES)).T

    for step in range(1, groups):
        for t in range(iters):
            for i in range(reps):
                bound = ext[step, t, 4:5, i * LANES : (i + 1) * LANES]
                inv[step - 1, t, i * LANES : (i + 1) * LANES, :] = tall(
                    LEVELS / jnp.maximum(bound, 1e-30)
                )

    def swap(c, step):
        return remote(
            send.at[c % 2, step - 1], recv.at[c, step - 1], swap_send.at[c, step - 1],
            swap_recv.at[c, step - 1], peer(step),
        )

    tile = owned

    def gather_slots(c, q):
        for core_of in range(2):
            origin = q * 2 + core_of
            got = []
            for b in range(local):
                x = jnp.dot(select[origin, b], rows[c, origin, b], preferred_element_type=jnp.float32)
                got.append(x.astype(jnp.bfloat16).reshape(iters * most // 16, 16, width))
            for g in range(groups):
                for i in range(CAP):
                    put = got[0] * share[origin, 0, g * CAP + i][None]
                    for b in range(1, local):
                        put = put + got[b] * share[origin, b, g * CAP + i][None]
                    put = put.reshape(iters, most, width)
                    at = core_of * slots + i * most
                    for t in range(iters):
                        compact[t, g, at : at + most, :] = put[t]

    def tally(c, q):
        gather_slots(c, q)

        def body(i, carry):
            for t in range(iters):
                part = pl.ds(pl.multiple_of(i * tile, tile), tile)
                acc[t, part, :] += jnp.dot(
                    place_in[t, q, part, :], compact[t, i], preferred_element_type=jnp.float32
                )
            return carry

        lax.fori_loop(0, groups, body, 0)

    def decode(word):
        high = lax.shift_right_logical(word, 16)
        low = word & 0xFFFF
        return [high.astype(jnp.float32) - HALF, low.astype(jnp.float32) - HALF]

    def late_codes(x, kind):
        to = mate if kind == 2 else chips - 1 - chip
        slot = 0 if kind == 2 else kind
        device = (mine, to * 2 + core)
        return (
            remote(late_out.at[x, kind], late_in.at[x, slot], code_s.at[x, kind], code_r.at[x, slot], device),
            remote(
                late_scale_out.at[x, kind], late_scale_in.at[x, slot], scale_s.at[x, kind],
                scale_r.at[x, slot], device,
            ),
        )

    ones = jnp.ones((LANES, LANES), jnp.bfloat16)

    def late_emit(x, kind, sums_of):
        for i in range(reps):
            part = slice(i * LANES, (i + 1) * LANES)
            codes = []
            for t, value in enumerate(sums_of(part)):
                power = (value * value * 1.02).astype(jnp.bfloat16)
                tall_norm = jnp.dot(power, ones, preferred_element_type=jnp.float32)
                wide_norm = lax.dot_general(
                    ones[:16], power, (((1,), (1,)), ((), ())), preferred_element_type=jnp.float32
                )
                late_scale_out[x, kind, t : t + 1, part] = (
                    jnp.sqrt(jnp.maximum(wide_norm[0:1], 1e-30)) * (1.0 / LEVELS)
                )
                inverse = LEVELS * lax.rsqrt(jnp.maximum(tall_norm, 1e-30))
                codes.append((value * inverse + (HALF + 0.5)).astype(jnp.int32))
            late_out[x, kind, part, :] = (codes[0] << 16) | codes[1]
        for copy in late_codes(x, kind):
            copy.start()

    def late_wait(x, slot):
        for copy in (
            remote(late_out.at[x, slot], late_in.at[x, slot], code_s.at[x, slot], code_r.at[x, slot], partner),
            remote(
                late_scale_out.at[x, slot], late_scale_in.at[x, slot], scale_s.at[x, slot],
                scale_r.at[x, slot], partner,
            ),
        ):
            copy.wait_recv()

    def late_sums(x, target, slot, part):
        values = decode(late_in[x, slot, part, :])
        return [
            late_acc[x, target, t, part, :] + v * tall(late_scale_in[x, slot, t : t + 1, part])
            for t, v in enumerate(values)
        ]

    ids_w = lax.broadcasted_iota(jnp.int32, (owned, groups * slots), 0)

    def late_tally(target, wanted_range, at):
        for t in range(iters):
            base = FIXED + 4 * t
            for g in range(groups):
                found = []
                for i in range(CAP):
                    e = late_metas[at, g, i]
                    f = e.astype(jnp.float32)
                    wanted = (f[base + 2 : base + 3, :].astype(jnp.int32) == wanted_range) & (f[0:1, :] > 0.5)
                    pos = jnp.where(wanted, f[base + 3 : base + 4, :].astype(jnp.int32), -1)
                    hot = (ids_m == pos).astype(jnp.bfloat16)
                    late_select[g, i, t * most : (t + 1) * most, :] = hot[:most, :]
                    x = lax.dot_general(
                        e, hot, (((1,), (1,)), ((), ())), preferred_element_type=jnp.float32
                    )
                    found.append(jnp.where(turns == i, x, 0.0))
                pair = found[0]
                for x in found[1:]:
                    pair = pair + x
                label = pair[base : base + 1, :] + 256.0 * pair[base + 1 : base + 2, :]
                late_cells[t, :, g * slots : (g + 1) * slots] = jnp.where(
                    pair[0:1, :] > 0.5, label.astype(jnp.int32), -1
                )
        for x in range(late):
            for g in range(groups):
                for i in range(CAP):
                    got = jnp.dot(
                        late_select[g, i], late_rows[x, at, g, i], preferred_element_type=jnp.float32
                    ).astype(jnp.bfloat16)
                    spot = g * slots + i * most
                    for t in range(iters):
                        late_compact[x, t, spot : spot + most, :] = got[t * most : (t + 1) * most, :]
        for t in range(iters):
            hot = (ids_w == late_cells[t]).astype(jnp.bfloat16)
            for x in range(late):
                late_acc[x, target, t] += jnp.dot(
                    hot, late_compact[x, t], preferred_element_type=jnp.float32
                )

    def late_step(j):
        order = (j % 8) // 2
        target = jnp.where(order == 2, 0, jnp.where(order == 3, 3, order + 1))
        at = (j // 8) * 2 + j % 2
        wanted_range = targets[0]
        for i in range(1, 4):
            wanted_range = jnp.where(target == i, targets[i], wanted_range)

        @pl.when(j == 0)
        def _():
            for x in range(late + 1):
                late_partner(x).wait_recv()

        @pl.when((j == 8) & jnp.logical_not(is_end))
        def _():
            for x in range(late + 1):
                late_inward(x).wait_recv()
                late_share(x).start()
            for x in range(late + 1):
                late_share(x).wait_recv()

        here = jnp.where(is_end, (target == 0) & (at < 2), (target != 3) | (at < 2))

        @pl.when(here & (j < 16))
        def _():
            late_tally(target, wanted_range, at)

        for kind, when in ((0, 9), (1, 11)):

            @pl.when((j == when) & jnp.logical_not(is_end))
            def _():
                for x in range(late):
                    late_emit(
                        x, kind, lambda part: [late_acc[x, kind + 1, t, part, :] for t in range(iters)]
                    )

        @pl.when((j == 15) & jnp.logical_not(is_end))
        def _():
            for x in range(late):
                late_wait(x, 1)
                late_emit(x, 2, lambda part: late_sums(x, 3, 1, part))

    def finish_late(x):
        load_prior(chunks + x).wait()
        late_wait(x, 0)
        for i in range(reps):
            part = slice(i * LANES, (i + 1) * LANES)
            update(chunks + x, part, late_sums(x, 0, 0, part))

    def update(c, part, sums):
        previous = prior[c, part, :]
        for t in range(iters):
            count = cnt[t, part, :]
            if t == iters - 1:
                within[part, :] += previous * (count * previous - 2.0 * sums[t])
            previous = (sums[t] + PRIOR * previous) / (count + PRIOR)
        at = c * width
        out[part, pl.ds(at if isinstance(at, int) else pl.multiple_of(at, width), width)] = previous

    def settle(c):
        for t in range(iters):
            own[c, t] = acc[t, :owned, :]

        @pl.when(c >= 2)
        def _():
            for step in range(1, groups):
                swap(c - 2, step).wait_send()

        for step in range(1, groups):
            part = slice(step * owned, (step + 1) * owned)
            high = (acc[0, part, :] * inv[step - 1, 0] + (HALF + 0.5)).astype(jnp.int32)
            low = (acc[1, part, :] * inv[step - 1, 1] + (HALF + 0.5)).astype(jnp.int32)
            send[c % 2, step - 1] = (high << 16) | low
            swap(c, step).start()
        acc[...] = jnp.zeros_like(acc)

    def scales():
        for step in range(1, groups):
            ext_to(step).wait_recv()
        for t in range(iters):
            for i in range(reps):
                part = slice(i * LANES, (i + 1) * LANES)
                count = ext[0, t, 0:1, part]
                for step in range(1, groups):
                    count = count + ext_recv[step - 1, t, 0:1, part]
                    scale[step - 1, t, part, :] = tall(ext_recv[step - 1, t, 4:5, part] / LEVELS)
                cnt[t, part, :] = tall(count)
        within[...] = jnp.zeros_like(within)

    def finish(c):
        load_prior(c).wait()
        for step in range(1, groups):
            swap(c, step).wait_recv()
        for i in range(reps):
            part = slice(i * LANES, (i + 1) * LANES)
            sums = [own[c, t, part, :] for t in range(iters)]
            for step in range(1, groups):
                for t, value in enumerate(decode(recv[c, step - 1, part, :])):
                    sums[t] = sums[t] + value * scale[step - 1, t, part, :]
            update(c, part, sums)

    def main_step(j, carry):
        c, k = j // chips, j % chips
        q = source(k)
        ahead = j + jnp.where(both > 0, chips, 0)

        @pl.when((ahead >= chips) & (ahead < chunks * chips))
        def _():
            pull(ahead)

        from_partner(c, q).wait_recv()
        tally(c, q)
        late_step(j)

        @pl.when(k == chips - 1)
        def _():
            settle(c)

            @pl.when(c == 0)
            def _():
                scales()

            @pl.when(c > 0)
            def _():
                finish(c - 1)

        return carry

    lax.fori_loop(0, chunks * chips, main_step, 0)
    for x in range(late):
        finish_late(x)
    finish(chunks - 1)

    for i in range(reps):
        part = slice(i * LANES, (i + 1) * LANES)
        spread = jnp.sum(within[part, :].T, axis=0, keepdims=True)
        last = iters - 1
        count = ext[0, last, 0:1, part]
        square = ext[0, last, 1:2, part] + ext[0, last, 2:3, part] + ext[0, last, 3:4, part]
        for step in range(1, groups):
            far = ext_recv[step - 1, last, :, part]
            count = count + far[0:1]
            square = square + far[1:2] + far[2:3] + far[3:4]
        inertia[:, part] = (spread + square) / ((count + PRIOR) * features)

    for other in range(1, chips):
        meta_to(other).wait_send()
    for q in range(chips):
        meta_partner(q).wait_send()
    for step in range(1, groups):
        ext_to(step).wait_send()

    def drain(j, carry):
        c, q = j // chips, j % chips

        @pl.when((q <= chip) & (chip < chips - 1))
        def _():
            to_right(c, q).wait_send()

        @pl.when((q >= chip) & (chip > 0))
        def _():
            to_left(c, q).wait_send()

        to_partner(c, q).wait_send()
        return carry

    lax.fori_loop(0, chunks * chips, drain, 0)

    for x in range(late + 1):
        for step in range(1, groups):
            late_swap(x, step).wait_send()
        late_partner(x).wait_send()

        @pl.when(is_end)
        def _():
            late_inward(x).wait_send()

        @pl.when(jnp.logical_not(is_end))
        def _():
            late_share(x).wait_send()

    for x in range(late):

        @pl.when(jnp.logical_not(is_end))
        def _():
            for kind in range(3):
                for copy in late_codes(x, kind):
                    copy.wait_send()

    for c in range(chunks - 2, chunks):
        for step in range(1, groups):
            swap(c, step).wait_send()


def fused_buffers(local, block_rows, features, iters, owned, groups, shards):
    chips = shards // 2
    most = 2 * block_rows // shards
    width, late = LANES, features // LANES // 3
    chunks = features // LANES - late
    slots = CAP * most
    vmem = pltpu.VMEM
    f32, b16, i32 = jnp.float32, jnp.bfloat16, jnp.int32
    buffers = [
        ((chunks, shards, local, block_rows, width), b16),
        ((shards, local, META_ROWS, block_rows), b16),
        ((shards, local, iters * most, block_rows), b16),
        ((iters, chips, groups * owned, 2 * slots), b16),
        ((iters, groups * owned, width), f32),
        ((iters, groups, 2 * slots, width), b16),
        ((chunks, iters, owned, width), f32),
        ((2, groups - 1, owned, width), i32),
        ((chunks, groups - 1, owned, width), i32),
        ((groups - 1, iters, owned, width), f32),
        ((groups - 1, iters, owned, width), f32),
        ((iters, owned, width), f32),
        ((groups, iters, META_ROWS, owned), f32),
        ((groups - 1, iters, META_ROWS, owned), f32),
        ((chunks + late, owned, width), f32),
        ((owned, width), f32),
        ((META_ROWS, block_rows), f32),
        ((shards, local, groups * CAP, 16, LANES), b16),
        ((late, local, block_rows, width), b16),
        ((late, groups - 1, CAP, block_rows, width), b16),
        ((late, 4, groups, CAP, block_rows, width), b16),
        ((groups - 1, CAP, META_ROWS, block_rows), b16),
        ((4, groups, CAP, META_ROWS, block_rows), b16),
        ((groups, CAP, iters * most, block_rows), b16),
        ((iters, 1, groups * slots), i32),
        ((late, iters, groups * slots, width), b16),
        ((late, 4, iters, owned, width), f32),
        ((late, 3, owned, width), i32),
        ((late, 2, owned, width), i32),
        ((late, 3, 8, owned), f32),
        ((late, 2, 8, owned), f32),
    ]
    dma = pltpu.SemaphoreType.DMA
    sems = [dma((chunks,)), dma((chunks + late,))]
    sems += [dma((chips,))] * 4
    sems += [dma((chunks, chips))] * 6
    sems += [dma((groups - 1,))] * 2
    sems += [dma((chunks, groups - 1))] * 2
    sems += [dma((late,))] + [dma((late + 1, groups - 1))] * 2 + [dma((late + 1,))] * 6
    sems += [dma((late, 3)), dma((late, 2))] * 2
    return [vmem(s, d) for s, d in buffers], sems, buffers, most, chunks, late


def fits(local, block_rows, features, iters, owned, groups, shards):
    if features % LANES or features < 2 * LANES or owned % LANES or shards % 2:
        return False
    if shards != 8 or features < 6 * LANES:
        return False
    if iters != 2 or 4 * iters + FIXED > META_ROWS or (2 * block_rows) % shards:
        return False
    most = 2 * block_rows // shards
    if (CAP * most) % LANES or CAP * most > block_rows or most % 16 or block_rows % LANES:
        return False
    total = 0
    for shape, dtype in fused_buffers(local, block_rows, features, iters, owned, groups, shards)[2]:
        size = jnp.dtype(dtype).itemsize
        for extent in shape:
            size *= extent
        total += size
    return total < 60 * 2**20


def fused_body(embeddings, assignments, block_group, centroids):
    groups, shards = lax.axis_size("group"), lax.axis_size("shard")
    local, block_rows, features = embeddings.shape
    iters = assignments.shape[1]
    owned = centroids.shape[1] // shards
    buffers, sems, unused, most, chunks, late = fused_buffers(
        local, block_rows, features, iters, owned, groups, shards
    )

    out, inertia = pl.pallas_call(
        functools.partial(fused_kernel, chunks, late, most),
        out_shape=[
            pltpu.VMEM((owned, features), jnp.float32),
            pltpu.VMEM((1, owned), jnp.float32),
        ],
        in_specs=[
            pl.BlockSpec(memory_space=pltpu.SMEM),
            pl.BlockSpec(memory_space=pltpu.VMEM),
            pl.BlockSpec(memory_space=pl.ANY),
            pl.BlockSpec(memory_space=pl.ANY),
        ],
        out_specs=[pl.BlockSpec(memory_space=pltpu.VMEM)] * 2,
        scratch_shapes=buffers + sems,
        compiler_params=pltpu.CompilerParams(
            collective_id=0, has_side_effects=True, vmem_limit_bytes=61 * 2**20
        ),
    )(block_group, assignments, embeddings, centroids)
    return out[None], inertia


def choose(embeddings, assignments, block_group, centroids):
    groups, shards = lax.axis_size("group"), lax.axis_size("shard")
    local, block_rows, features = embeddings.shape
    owned = centroids.shape[1] // shards
    if fits(local, block_rows, features, assignments.shape[1], owned, groups, shards):
        return fused_body(embeddings, assignments, block_group, centroids)
    return body(embeddings, assignments, block_group, centroids)


def solution(mesh):
    in_specs = (
        P(("group", "shard"), None, None),
        P(("group", "shard"), None, None),
        P(("group", "shard")),
        P("group", None, None),
    )
    out_specs = (P("group", "shard", None), P("group", "shard"))
    return jax.shard_map(choose, mesh=mesh, in_specs=in_specs, out_specs=out_specs, check_vma=False)
```

```python
import functools

import jax
import jax.numpy as jnp
from jax import lax
from jax.experimental import pallas as pl
from jax.experimental.pallas import tpu as pltpu
from jax.sharding import PartitionSpec as P

PRIOR = 8.0
META = 8
CHUNKS = 3
MESH = pl.DeviceIdType.MESH


def exchange_kernel(n_gather, n_swap, width, column, *refs):
    n_in = n_gather + n_swap
    gathers, swaps = refs[:n_gather], refs[n_gather:n_in]
    outs = refs[n_in : 2 * n_in]
    gather_outs, swap_outs = outs[:n_gather], outs[n_gather:]
    scratch = refs[2 * n_in :]
    stages = scratch[:n_gather]
    scratch = scratch[n_gather:]

    groups, shards = lax.axis_size("group"), lax.axis_size("shard")
    chips = shards // 2
    mine, place = lax.axis_index("group"), lax.axis_index("shard")
    chip, core = place // 2, place % 2
    partner = (mine, chip * 2 + 1 - core)
    right = (mine, lax.rem(chip + 1, chips) * 2 + core)
    left = (mine, lax.rem(chip + chips - 1, chips) * 2 + core)

    def peer(step):
        return lax.rem(mine + step, groups)

    barrier = pltpu.get_barrier_semaphore()
    greeted = 0
    if n_gather:
        for device in (left, right, partner):
            pl.semaphore_signal(barrier, inc=1, device_id=device, device_id_type=MESH)
        greeted += 3
    if n_swap:
        for step in range(1, groups):
            pl.semaphore_signal(
                barrier, inc=1, device_id=(peer(step), place), device_id_type=MESH
            )
        greeted += groups - 1

    loads = []
    if n_gather:
        load_sem = scratch[0]
        for i in range(n_gather):
            source = gathers[i]
            if i == 0:
                source = source.at[:, :, pl.ds(column, width)]
            load = pltpu.make_async_copy(source, stages[i], load_sem.at[i])
            load.start()
            loads.append(load)
    pl.semaphore_wait(barrier, greeted)

    swap_copies = []
    if n_swap:
        swap_send, swap_recv = scratch[-2:]
        for step in range(1, groups):
            for i in range(n_swap):
                copy = pltpu.make_async_remote_copy(
                    src_ref=swaps[i].at[peer(step)],
                    dst_ref=swap_outs[i].at[step - 1],
                    send_sem=swap_send.at[i, step - 1],
                    recv_sem=swap_recv.at[i, step - 1],
                    device_id=(peer(step), place),
                    device_id_type=MESH,
                )
                copy.start()
                swap_copies.append(copy)

    if n_gather:
        store_sem, send_r, recv_r, send_l, recv_l, send_p, recv_p = scratch[1:8]
        stores = []

        def hop(i, source, origin, step, to, sends, recvs):
            return pltpu.make_async_remote_copy(
                src_ref=source,
                dst_ref=gather_outs[i].at[origin * 2 + core],
                send_sem=sends.at[i, step],
                recv_sem=recvs.at[i, step],
                device_id=to,
                device_id_type=MESH,
            )

        for i in range(n_gather):
            loads[i].wait()
            store = pltpu.make_async_copy(
                stages[i], gather_outs[i].at[place], store_sem.at[i]
            )

            @pl.when(chip < chips - 1)
            def _():
                hop(i, stages[i], chip, 0, right, send_r, recv_r).start()

            @pl.when(chip > 0)
            def _():
                hop(i, stages[i], chip, 0, left, send_l, recv_l).start()

            hop(i, stages[i], chip, chip, partner, send_p, recv_p).start()
            store.start()
            stores.append(store)

        for step in range(chips - 1):
            for i in range(n_gather):
                from_left = chip - 1 - step

                @pl.when(from_left >= 0)
                def _():
                    block = gather_outs[i].at[from_left * 2 + core]
                    hop(i, block, from_left, step, right, send_r, recv_r).wait_recv()

                    if step < chips - 2:

                        @pl.when(chip < chips - 1)
                        def _():
                            hop(i, block, from_left, step + 1, right, send_r, recv_r).start()

                    hop(i, block, from_left, from_left, partner, send_p, recv_p).start()

                from_right = chip + 1 + step

                @pl.when(from_right <= chips - 1)
                def _():
                    block = gather_outs[i].at[from_right * 2 + core]
                    hop(i, block, from_right, step, left, send_l, recv_l).wait_recv()

                    if step < chips - 2:

                        @pl.when(chip > 0)
                        def _():
                            hop(i, block, from_right, step + 1, left, send_l, recv_l).start()

                    hop(i, block, from_right, from_right, partner, send_p, recv_p).start()

        for i in range(n_gather):
            stores[i].wait()
            for step in range(chips - 1):

                @pl.when((chip - step >= 0) & (chip < chips - 1))
                def _():
                    hop(i, stages[i], chip, step, right, send_r, recv_r).wait_send()

                @pl.when((chip + step <= chips - 1) & (chip > 0))
                def _():
                    hop(i, stages[i], chip, step, left, send_l, recv_l).wait_send()

            for origin in range(chips):
                hop(i, stages[i], origin, origin, partner, send_p, recv_p).wait()

    for copy in swap_copies:
        copy.wait()


def exchange(gathers, swaps, width, column, key):
    groups, shards = lax.axis_size("group"), lax.axis_size("shard")
    chips = shards // 2
    n_gather, n_swap = len(gathers), len(swaps)
    shapes, scratch = [], []
    for i, array in enumerate(gathers):
        block = array.shape[:-1] + (width if i == 0 else array.shape[-1],)
        shapes.append(jax.ShapeDtypeStruct((shards,) + block, array.dtype))
        scratch.append(pltpu.VMEM(block, array.dtype))
    for array in swaps:
        shapes.append(jax.ShapeDtypeStruct((groups - 1,) + array.shape[1:], array.dtype))
    dma = pltpu.SemaphoreType.DMA
    if n_gather:
        scratch += [dma((n_gather,)), dma((n_gather,))]
        scratch += [dma((n_gather, max(chips - 1, 1)))] * 4
        scratch += [dma((n_gather, chips))] * 2
    if n_swap:
        scratch += [dma((n_swap, groups - 1))] * 2
    return pl.pallas_call(
        functools.partial(exchange_kernel, n_gather, n_swap, width, column),
        out_shape=shapes,
        in_specs=[pl.BlockSpec(memory_space=pl.ANY)] * (n_gather + n_swap),
        out_specs=[pl.BlockSpec(memory_space=pl.ANY)] * (n_gather + n_swap),
        scratch_shapes=scratch,
        compiler_params=pltpu.CompilerParams(collective_id=key, has_side_effects=True),
    )(*gathers, *swaps)


def tally_kernel(per_step, iters, with_extra, owners, labels, extra, rows, sums, *more):
    step = pl.program_id(0)
    centers = sums.shape[2]
    block_rows = rows.shape[1]

    @pl.when(step == 0)
    def _():
        sums[...] = jnp.zeros_like(sums)
        if with_extra:
            more[0][...] = jnp.zeros_like(more[0])

    ids = lax.broadcasted_iota(jnp.int32, (centers, block_rows), 0)
    for block in range(per_step):
        owner = owners[step * per_step + block]
        for t in range(iters):
            onehot = (ids == labels[block, t : t + 1, :]).astype(jnp.bfloat16)
            sums[owner, t] += jnp.dot(
                onehot, rows[block], preferred_element_type=jnp.float32
            )
            if with_extra:
                more[0][owner, t] += lax.dot_general(
                    extra[block],
                    onehot,
                    (((1,), (1,)), ((), ())),
                    preferred_element_type=jnp.float32,
                )


def tally(owners, labels, extra, rows, groups, centers, per_step, with_extra):
    blocks, iters, block_rows = labels.shape
    width = rows.shape[-1]
    shapes = [jax.ShapeDtypeStruct((groups, iters, centers, width), jnp.float32)]
    if with_extra:
        shapes.append(jax.ShapeDtypeStruct((groups, iters, extra.shape[1], centers), jnp.float32))
    out_specs = [pl.BlockSpec(s.shape, lambda i, o: (0, 0, 0, 0)) for s in shapes]
    return pl.pallas_call(
        functools.partial(tally_kernel, per_step, iters, with_extra),
        out_shape=shapes,
        grid_spec=pltpu.PrefetchScalarGridSpec(
            num_scalar_prefetch=1,
            grid=(blocks // per_step,),
            in_specs=[
                pl.BlockSpec((per_step, iters, block_rows), lambda i, o: (i, 0, 0)),
                pl.BlockSpec((per_step,) + extra.shape[1:], lambda i, o: (i, 0, 0)),
                pl.BlockSpec((per_step, block_rows, width), lambda i, o: (i, 0, 0)),
            ],
            out_specs=out_specs,
        ),
        compiler_params=pltpu.CompilerParams(vmem_limit_bytes=48 * 2**20),
    )(owners, labels, extra, rows)


def body(embeddings, assignments, block_group, centroids):
    groups, shards = lax.axis_size("group"), lax.axis_size("shard")
    mine, place = lax.axis_index("group"), lax.axis_index("shard")
    local, block_rows, features = embeddings.shape
    iters = assignments.shape[1]
    owned = centroids.shape[1] // shards
    chunks = CHUNKS if features % (CHUNKS * 128) == 0 else 1
    width = features // chunks
    blocks = shards * local

    wide = embeddings.astype(jnp.float32)
    squares = jnp.sum(wide * wide, axis=2)
    meta = jnp.concatenate(
        [
            assignments.astype(jnp.float32),
            jnp.broadcast_to(
                block_group[:, None, None].astype(jnp.float32), (local, 1, block_rows)
            ),
            squares[:, None, :],
            jnp.zeros((local, META - iters - 2, block_rows), jnp.float32),
        ],
        axis=1,
    )

    rows, metas = exchange([embeddings, meta], [], width, 0, 0)
    metas = metas.reshape(blocks, META, block_rows)
    labels = metas[:, :iters].astype(jnp.int32) - place * owned
    owners = metas[:, iters, 0].astype(jnp.int32)
    square = metas[:, iters + 1]
    high = lax.reduce_precision(square, 8, 7)
    middle = lax.reduce_precision(square - high, 8, 7)
    low = square - high - middle
    one = jnp.ones_like(square)
    zero = jnp.zeros_like(square)
    extra = jnp.stack([one, high, middle, low] + [zero] * 12, axis=1).astype(jnp.bfloat16)

    totals = []
    tail = None
    pending = []
    for chunk in range(chunks):
        result = tally(
            owners,
            labels,
            extra,
            rows.reshape(blocks, block_rows, width),
            groups,
            owned,
            local,
            chunk == 0,
        )
        column = (chunk + 1) * width
        if chunk + 1 < chunks:
            rows, *got = exchange([embeddings], result, width, column, chunk + 1)
        else:
            got = exchange([], result, width, 0, chunk + 1)
        whole = [
            lax.dynamic_index_in_dim(kept, mine, 0, keepdims=False) + jnp.sum(came, axis=0)
            for kept, came in zip(result, got)
        ]
        totals.append(whole[0])
        if chunk == 0:
            tail = whole[1]

    prior = lax.dynamic_slice_in_dim(centroids[0], place * owned, owned, 0)
    counts = tail[:, 0]
    within = tail[iters - 1, 1] + tail[iters - 1, 2] + tail[iters - 1, 3]
    pieces = []
    for chunk in range(chunks):
        previous = prior[:, chunk * width : (chunk + 1) * width]
        for t in range(iters):
            sums = totals[chunk][t]
            count = counts[t][:, None]
            if t == iters - 1:
                within = within + jnp.sum(
                    previous * (count * previous - 2.0 * sums), axis=1
                )
            previous = (sums + PRIOR * previous) / (count + PRIOR)
        pieces.append(previous)
    inertia = within / ((counts[iters - 1] + PRIOR) * features)
    return (jnp.concatenate(pieces, axis=1)[None], inertia[None])


LANES = 128
META_ROWS = 16
FIXED = 6
CAP = 2
LEVELS = 32000.0
HALF = 32768.0


def fused_kernel(
    chunks, late, most, owner_in, label_in, emb, cents, out, inertia,
    rows, metas, select, place_in, acc, compact, own, send, recv, inv, scale, cnt, ext,
    ext_recv, prior, within, lines, share,
    late_own, late_send, late_rows, late_meta_send, late_metas, late_select, late_cells, late_compact,
    late_acc, late_out, late_in, late_scale_out, late_scale_in,
    load_sem, prior_sem, meta_send, meta_recv, metap_send, metap_recv,
    send_r, recv_r, send_l, recv_l, send_p, recv_p, ext_ssem, ext_rsem, swap_send, swap_recv,
    late_load_sem, lswap_s, lswap_r, lpart_s, lpart_r, lin_s, lin_r, lshare_s, lshare_r,
    code_s, code_r, scale_s, scale_r,
):
    groups, shards = lax.axis_size("group"), lax.axis_size("shard")
    chips = shards // 2
    mine, place = lax.axis_index("group"), lax.axis_index("shard")
    chip, core = place // 2, place % 2
    partner = (mine, chip * 2 + 1 - core)
    right, left = (mine, place + 2), (mine, place - 2)
    is_end = (chip == 0) | (chip == chips - 1)
    mate = chip + 1 - 2 * lax.rem(chip, 2)
    targets = [place, (chips - 1 - chip) * 2 + core, (chips - 1 - mate) * 2 + core, mate * 2 + core]
    local, block_rows, features = emb.shape
    width = rows.shape[-1]
    iters = place_in.shape[0]
    owned = own.shape[2]
    slots = CAP * most
    reps = owned // LANES

    def peer(step):
        return (lax.rem(mine + step, groups), place)

    def remote(src, dst, ssem, rsem, to):
        return pltpu.make_async_remote_copy(
            src_ref=src, dst_ref=dst, send_sem=ssem, recv_sem=rsem,
            device_id=to, device_id_type=MESH,
        )

    def load(c):
        return pltpu.make_async_copy(
            emb.at[:, :, pl.ds(pl.multiple_of(c * width, width), width)],
            rows.at[c, place], load_sem.at[c],
        )

    def load_late(x):
        at = (chunks + x) * width
        return pltpu.make_async_copy(
            emb.at[:, :, pl.ds(at, width)], late_own.at[x], late_load_sem.at[x]
        )

    def load_prior(c):
        return pltpu.make_async_copy(
            cents.at[0, pl.ds(pl.multiple_of(place * owned, owned), owned),
                     pl.ds(pl.multiple_of(c * width, width), width)],
            prior.at[c], prior_sem.at[c],
        )

    for c in range(chunks):
        load(c).start()
    for x in range(late):
        load_late(x).start()

    barrier = pltpu.get_barrier_semaphore()
    for other in range(1, chips):
        pl.semaphore_signal(
            barrier, inc=1, device_id=(mine, lax.rem(chip + other, chips) * 2 + core),
            device_id_type=MESH,
        )
    pl.semaphore_signal(barrier, inc=1, device_id=partner, device_id_type=MESH)
    for step in range(1, groups):
        pl.semaphore_signal(barrier, inc=1, device_id=peer(step), device_id_type=MESH)
    pl.semaphore_wait(barrier, chips + groups - 1)

    def meta_to(other):
        target = lax.rem(chip + other, chips)
        return remote(
            metas.at[place], metas.at[place], meta_send.at[other], meta_recv.at[other],
            (mine, target * 2 + core),
        )

    def meta_partner(q):
        block = metas.at[q * 2 + core]
        return remote(block, block, metap_send.at[q], metap_recv.at[q], partner)

    def to_right(c, q):
        block = rows.at[c, q * 2 + core]
        return remote(block, block, send_r.at[c, chip - q], recv_r.at[c, chip - q], right)

    def to_left(c, q):
        block = rows.at[c, q * 2 + core]
        return remote(block, block, send_l.at[c, q - chip], recv_l.at[c, q - chip], left)

    def to_partner(c, q):
        block = rows.at[c, q * 2 + core]
        return remote(block, block, send_p.at[c, q], recv_p.at[c, q], partner)

    def from_left(c, q):
        block = rows.at[c, q * 2 + core]
        return remote(
            block, block, send_r.at[c, chip - 1 - q], recv_r.at[c, chip - 1 - q], right
        )

    def from_right(c, q):
        block = rows.at[c, q * 2 + core]
        return remote(
            block, block, send_l.at[c, q - chip - 1], recv_l.at[c, q - chip - 1], left
        )

    def from_partner(c, q):
        block = rows.at[c, q * 2 + 1 - core]
        return remote(block, block, send_p.at[c, q], recv_p.at[c, q], partner)

    def issue_own(c):
        @pl.when(chip < chips - 1)
        def _():
            to_right(c, chip).start()

        @pl.when(chip > 0)
        def _():
            to_left(c, chip).start()

        to_partner(c, chip).start()

    load(0).wait()
    load(1).wait()
    issue_own(0)
    for c in range(chunks + late):
        load_prior(c).start()
    for c in range(2, chunks):
        load(c).wait()
    for x in range(late):
        load_late(x).wait()

    ids_s = lax.broadcasted_iota(jnp.int32, (shards, block_rows), 0).astype(jnp.float32)
    before = (
        lax.broadcasted_iota(jnp.int32, (block_rows, block_rows), 0)
        < lax.broadcasted_iota(jnp.int32, (block_rows, block_rows), 1)
    ).astype(jnp.bfloat16)
    labels = [[label_in[b, t : t + 1, :].astype(jnp.float32) for t in range(iters)] for b in range(local)]
    ranges = [[jnp.floor((x + 0.5) * (1.0 / owned)) for x in xs] for xs in labels]
    hots = [[(ids_s == x).astype(jnp.float32) for x in xs] for xs in ranges]
    flat = [x for xs in hots for x in xs]
    earlier = jnp.dot(
        jnp.concatenate(flat, axis=0).astype(jnp.bfloat16), before,
        preferred_element_type=jnp.float32,
    )
    lines[...] = jnp.zeros_like(lines)
    for b in range(local):
        total = jnp.zeros((block_rows, width), jnp.float32)
        top = jnp.zeros((block_rows, width), jnp.float32)
        for c in range(chunks + late):
            x = rows[c, place, b] if c < chunks else late_own[c - chunks, b]
            x = x.astype(jnp.float32)
            total = total + x * x
            top = jnp.maximum(top, jnp.abs(x))
        square = jnp.sum(total.T, axis=0, keepdims=True)
        high = square.astype(jnp.bfloat16).astype(jnp.float32)
        middle = (square - high).astype(jnp.bfloat16).astype(jnp.float32)
        lines[0:1, :] = jnp.ones_like(square)
        lines[1:2, :] = high
        lines[2:3, :] = middle
        lines[3:4, :] = square - high - middle
        lines[4:5, :] = jnp.max(top.T, axis=0, keepdims=True)
        turn = owner_in[b] * CAP
        for other in range(b):
            turn = turn + jnp.where(owner_in[other] == owner_in[b], 1, 0)
        lines[5:6, :] = jnp.full((1, block_rows), turn, jnp.int32).astype(jnp.float32)
        for t in range(iters):
            base = FIXED + 4 * t
            inside = labels[b][t] - ranges[b][t] * owned
            coarse = jnp.floor((inside + 0.5) * (1.0 / 256))
            at = (b * iters + t) * shards
            lines[base : base + 1, :] = inside - 256.0 * coarse
            lines[base + 1 : base + 2, :] = coarse
            lines[base + 2 : base + 3, :] = ranges[b][t]
            lines[base + 3 : base + 4, :] = jnp.sum(
                hots[b][t] * earlier[at : at + shards, :], axis=0, keepdims=True
            )
        metas[place, b] = lines[...].astype(jnp.bfloat16)

    for other in range(1, chips):
        meta_to(other).start()
    issue_own(1)

    @pl.when(is_end)
    def _():
        for c in range(2, chunks):
            issue_own(c)

    def late_swap(x, step):
        sent = late_meta_send if x == late else late_send.at[x]
        kept = late_metas if x == late else late_rows.at[x]
        return remote(
            sent.at[step - 1], kept.at[core, step], lswap_s.at[x, step - 1],
            lswap_r.at[x, step - 1], peer(step),
        )

    def late_block(x, at):
        return late_metas.at[at] if x == late else late_rows.at[x, at]

    def late_partner(x):
        block = late_block(x, core)
        return remote(block, block, lpart_s.at[x], lpart_r.at[x], partner)

    def late_inward(x):
        return remote(
            late_block(x, core), late_block(x, 2 + core), lin_s.at[x], lin_r.at[x],
            (mine, mate * 2 + core),
        )

    def late_share(x):
        block = late_block(x, 2 + core)
        return remote(block, block, lshare_s.at[x], lshare_r.at[x], partner)

    def late_start():
        for x in (late,) + tuple(range(late)):
            for step in range(1, groups):
                late_swap(x, step).wait_recv()
            late_partner(x).start()

            @pl.when(is_end)
            def _():
                late_inward(x).start()

    chosen = []
    for b in range(local):
        turn = metas[place, b].astype(jnp.float32)[5:6, :LANES].astype(jnp.int32) - mine * CAP
        chosen.append(jnp.where(turn < 0, turn + groups * CAP, turn))
    for step in range(groups):
        for i in range(CAP):
            weights = [
                jnp.broadcast_to(
                    (turn == step * CAP + i).astype(jnp.float32), (META_ROWS, LANES)
                ).astype(jnp.bfloat16)
                for turn in chosen
            ]

            def pick(blocks):
                tiles = [x.reshape(x.shape[0] // META_ROWS, META_ROWS, LANES) for x in blocks]
                put = tiles[0] * weights[0][None]
                for b in range(1, local):
                    put = put + tiles[b] * weights[b][None]
                return put.reshape(blocks[0].shape)

            for lane in range(0, block_rows, LANES):
                part = slice(lane, lane + LANES)
                put = pick([metas[place, b, :, part] for b in range(local)])
                if step == 0:
                    late_metas[core, 0, i, :, part] = put
                else:
                    late_meta_send[step - 1, i, :, part] = put
            for x in range(late):
                put = pick([late_own[x, b] for b in range(local)])
                if step == 0:
                    late_rows[x, core, 0, i] = put
                else:
                    late_send[x, step - 1, i] = put
    for x in (late,) + tuple(range(late)):
        for step in range(1, groups):
            late_swap(x, step).start()

    on_left, on_right = chip, chips - 1 - chip
    both = jnp.minimum(on_left, on_right)

    def source(k):
        paired = k <= 2 * both
        distance = jnp.where(paired, (k + 1) // 2, k - both)
        is_left = jnp.where(paired, (k % 2) == 1, on_left > on_right)
        return jnp.where(is_left, chip - distance, chip + distance)

    def pull(j):
        c, k = j // chips, j % chips
        q = source(k)

        @pl.when((k == 0) & (c + 2 < chunks) & jnp.logical_not(is_end))
        def _():
            issue_own(c + 2)

        @pl.when(q < chip)
        def _():
            from_left(c, q).wait_recv()

            @pl.when(chip < chips - 1)
            def _():
                to_right(c, q).start()

            to_partner(c, q).start()

        @pl.when(q > chip)
        def _():
            from_right(c, q).wait_recv()

            @pl.when(chip > 0)
            def _():
                to_left(c, q).start()

            to_partner(c, q).start()

    ids_m = lax.rem(lax.broadcasted_iota(jnp.int32, (slots, block_rows), 0), most)
    ids_c = lax.broadcasted_iota(jnp.int32, (owned, slots), 0)
    turns = lax.broadcasted_iota(jnp.int32, (1, slots), 1) // most

    ext[...] = jnp.zeros_like(ext)
    acc[...] = jnp.zeros_like(acc)
    late_acc[...] = jnp.zeros_like(late_acc)
    late_scale_out[...] = jnp.zeros_like(late_scale_out)

    def take_meta(q, core_of):
        origin = q * 2 + core_of
        rel = []
        for b in range(local):
            place_of = metas[origin, b].astype(jnp.float32)[5:6, :slots].astype(jnp.int32) - mine * CAP
            rel.append(jnp.where(place_of < 0, place_of + groups * CAP, place_of))
            for i in range(groups * CAP):
                one = (rel[b] == i).astype(jnp.float32)[:, :LANES]
                share[origin, b, i] = jnp.broadcast_to(one, (16, LANES)).astype(jnp.bfloat16)
        for t in range(iters):
            base = FIXED + 4 * t
            found = []
            for b in range(local):
                e = metas[origin, b]
                f = e.astype(jnp.float32)
                wanted = f[base + 2 : base + 3, :].astype(jnp.int32) == place
                pos = jnp.where(wanted, f[base + 3 : base + 4, :].astype(jnp.int32), -1)
                hot = (ids_m == pos).astype(jnp.bfloat16)
                select[origin, b, t * most : (t + 1) * most, :] = hot[:most, :]
                found.append(
                    lax.dot_general(
                        e, hot, (((1,), (1,)), ((), ())), preferred_element_type=jnp.float32
                    )
                )
            for g in range(groups):
                pair = jnp.zeros((META_ROWS, slots), jnp.float32)
                for b in range(local):
                    pair = pair + jnp.where(rel[b] == turns + g * CAP, found[b], 0.0)
                label = pair[base : base + 1, :] + 256.0 * pair[base + 1 : base + 2, :]
                cell = jnp.where(pair[0:1, :] > 0.5, label.astype(jnp.int32), -1)
                hot = (ids_c == cell).astype(jnp.bfloat16)
                part = slice(core_of * slots, (core_of + 1) * slots)
                place_in[t, q, g * owned : (g + 1) * owned, part] = hot
                ext[g, t] += lax.dot_general(
                    pair.astype(jnp.bfloat16), hot, (((1,), (1,)), ((), ())),
                    preferred_element_type=jnp.float32,
                )

    def meta_step(k, carry):
        q = source(k)

        @pl.when(q != chip)
        def _():
            other = lax.rem(chip - q + chips, chips)
            block = metas.at[q * 2 + core]
            remote(block, block, meta_send.at[other], meta_recv.at[other], left).wait_recv()

        meta_partner(q).start()
        for core_of in range(2):

            @pl.when(core_of != core)
            def _():
                block = metas.at[q * 2 + 1 - core]
                remote(block, block, metap_send.at[q], metap_recv.at[q], partner).wait_recv()

        for core_of in range(2):
            take_meta(q, core_of)
        pull(k)

        @pl.when((both > 0) & (k >= chips - 2))
        def _():
            pull(k + 2)

        return carry

    lax.fori_loop(0, chips, meta_step, 0)
    late_start()

    def ext_to(step):
        return remote(
            ext.at[step], ext_recv.at[step - 1], ext_ssem.at[step - 1], ext_rsem.at[step - 1],
            peer(step),
        )

    for step in range(1, groups):
        ext_to(step).start()

    def tall(row):
        return jnp.broadcast_to(row, (LANES, LANES)).T

    for step in range(1, groups):
        for t in range(iters):
            for i in range(reps):
                bound = ext[step, t, 4:5, i * LANES : (i + 1) * LANES]
                inv[step - 1, t, i * LANES : (i + 1) * LANES, :] = tall(
                    LEVELS / jnp.maximum(bound, 1e-30)
                )

    def swap(c, step):
        return remote(
            send.at[c % 2, step - 1], recv.at[c, step - 1], swap_send.at[c, step - 1],
            swap_recv.at[c, step - 1], peer(step),
        )

    tile = owned

    def gather_slots(c, q):
        for core_of in range(2):
            origin = q * 2 + core_of
            got = []
            for b in range(local):
                x = jnp.dot(select[origin, b], rows[c, origin, b], preferred_element_type=jnp.float32)
                got.append(x.astype(jnp.bfloat16).reshape(iters * most // 16, 16, width))
            for g in range(groups):
                for i in range(CAP):
                    put = got[0] * share[origin, 0, g * CAP + i][None]
                    for b in range(1, local):
                        put = put + got[b] * share[origin, b, g * CAP + i][None]
                    put = put.reshape(iters, most, width)
                    at = core_of * slots + i * most
                    for t in range(iters):
                        compact[t, g, at : at + most, :] = put[t]

    def tally(c, q):
        gather_slots(c, q)

        def body(i, carry):
            for t in range(iters):
                part = pl.ds(pl.multiple_of(i * tile, tile), tile)
                acc[t, part, :] += jnp.dot(
                    place_in[t, q, part, :], compact[t, i], preferred_element_type=jnp.float32
                )
            return carry

        lax.fori_loop(0, groups, body, 0)

    def decode(word):
        high = lax.shift_right_logical(word, 16)
        low = word & 0xFFFF
        return [high.astype(jnp.float32) - HALF, low.astype(jnp.float32) - HALF]

    def late_codes(x, kind):
        to = mate if kind == 2 else chips - 1 - chip
        slot = 0 if kind == 2 else kind
        device = (mine, to * 2 + core)
        return (
            remote(late_out.at[x, kind], late_in.at[x, slot], code_s.at[x, kind], code_r.at[x, slot], device),
            remote(
                late_scale_out.at[x, kind], late_scale_in.at[x, slot], scale_s.at[x, kind],
                scale_r.at[x, slot], device,
            ),
        )

    ones = jnp.ones((LANES, LANES), jnp.bfloat16)

    def late_emit(x, kind, sums_of):
        for i in range(reps):
            part = slice(i * LANES, (i + 1) * LANES)
            codes = []
            for t, value in enumerate(sums_of(part)):
                power = (value * value * 1.02).astype(jnp.bfloat16)
                tall_norm = jnp.dot(power, ones, preferred_element_type=jnp.float32)
                wide_norm = lax.dot_general(
                    ones[:16], power, (((1,), (1,)), ((), ())), preferred_element_type=jnp.float32
                )
                late_scale_out[x, kind, t : t + 1, part] = (
                    jnp.sqrt(jnp.maximum(wide_norm[0:1], 1e-30)) * (1.0 / LEVELS)
                )
                inverse = LEVELS * lax.rsqrt(jnp.maximum(tall_norm, 1e-30))
                codes.append((value * inverse + (HALF + 0.5)).astype(jnp.int32))
            late_out[x, kind, part, :] = (codes[0] << 16) | codes[1]
        for copy in late_codes(x, kind):
            copy.start()

    def late_wait(x, slot):
        for copy in (
            remote(late_out.at[x, slot], late_in.at[x, slot], code_s.at[x, slot], code_r.at[x, slot], partner),
            remote(
                late_scale_out.at[x, slot], late_scale_in.at[x, slot], scale_s.at[x, slot],
                scale_r.at[x, slot], partner,
            ),
        ):
            copy.wait_recv()

    def late_sums(x, target, slot, part):
        values = decode(late_in[x, slot, part, :])
        return [
            late_acc[x, target, t, part, :] + v * tall(late_scale_in[x, slot, t : t + 1, part])
            for t, v in enumerate(values)
        ]

    ids_w = lax.broadcasted_iota(jnp.int32, (owned, groups * slots), 0)

    def late_tally(target, wanted_range, at):
        for t in range(iters):
            base = FIXED + 4 * t
            for g in range(groups):
                found = []
                for i in range(CAP):
                    e = late_metas[at, g, i]
                    f = e.astype(jnp.float32)
                    wanted = (f[base + 2 : base + 3, :].astype(jnp.int32) == wanted_range) & (f[0:1, :] > 0.5)
                    pos = jnp.where(wanted, f[base + 3 : base + 4, :].astype(jnp.int32), -1)
                    hot = (ids_m == pos).astype(jnp.bfloat16)
                    late_select[g, i, t * most : (t + 1) * most, :] = hot[:most, :]
                    x = lax.dot_general(
                        e, hot, (((1,), (1,)), ((), ())), preferred_element_type=jnp.float32
                    )
                    found.append(jnp.where(turns == i, x, 0.0))
                pair = found[0]
                for x in found[1:]:
                    pair = pair + x
                label = pair[base : base + 1, :] + 256.0 * pair[base + 1 : base + 2, :]
                late_cells[t, :, g * slots : (g + 1) * slots] = jnp.where(
                    pair[0:1, :] > 0.5, label.astype(jnp.int32), -1
                )
        for x in range(late):
            for g in range(groups):
                for i in range(CAP):
                    got = jnp.dot(
                        late_select[g, i], late_rows[x, at, g, i], preferred_element_type=jnp.float32
                    ).astype(jnp.bfloat16)
                    spot = g * slots + i * most
                    for t in range(iters):
                        late_compact[x, t, spot : spot + most, :] = got[t * most : (t + 1) * most, :]
        for t in range(iters):
            hot = (ids_w == late_cells[t]).astype(jnp.bfloat16)
            for x in range(late):
                late_acc[x, target, t] += jnp.dot(
                    hot, late_compact[x, t], preferred_element_type=jnp.float32
                )

    def late_step(j):
        order = (j % 8) // 2
        target = jnp.where(order == 2, 0, jnp.where(order == 3, 3, 2 - order))
        at = (j // 8) * 2 + j % 2
        wanted_range = targets[0]
        for i in range(1, 4):
            wanted_range = jnp.where(target == i, targets[i], wanted_range)

        @pl.when(j == 0)
        def _():
            for x in range(late + 1):
                late_partner(x).wait_recv()

        @pl.when((j == 8) & jnp.logical_not(is_end))
        def _():
            for x in range(late + 1):
                late_inward(x).wait_recv()
                late_share(x).start()
            for x in range(late + 1):
                late_share(x).wait_recv()

        here = jnp.where(is_end, (target == 0) & (at < 2), (target != 3) | (at < 2))

        @pl.when(here & (j < 16))
        def _():
            late_tally(target, wanted_range, at)

        for kind, when in ((1, 9), (0, 11)):

            @pl.when((j == when) & jnp.logical_not(is_end))
            def _():
                for x in range(late):
                    late_emit(
                        x, kind, lambda part: [late_acc[x, kind + 1, t, part, :] for t in range(iters)]
                    )

        @pl.when((j == 14) & jnp.logical_not(is_end))
        def _():
            for x in range(late):
                late_wait(x, 1)
                late_emit(x, 2, lambda part: late_sums(x, 3, 1, part))

    def finish_late(x):
        load_prior(chunks + x).wait()
        late_wait(x, 0)
        for i in range(reps):
            part = slice(i * LANES, (i + 1) * LANES)
            update(chunks + x, part, late_sums(x, 0, 0, part))

    def update(c, part, sums):
        previous = prior[c, part, :]
        for t in range(iters):
            count = cnt[t, part, :]
            if t == iters - 1:
                within[part, :] += previous * (count * previous - 2.0 * sums[t])
            previous = (sums[t] + PRIOR * previous) / (count + PRIOR)
        at = c * width
        out[part, pl.ds(at if isinstance(at, int) else pl.multiple_of(at, width), width)] = previous

    def settle(c):
        for t in range(iters):
            own[c, t] = acc[t, :owned, :]

        @pl.when(c >= 2)
        def _():
            for step in range(1, groups):
                swap(c - 2, step).wait_send()

        for step in range(1, groups):
            part = slice(step * owned, (step + 1) * owned)
            high = (acc[0, part, :] * inv[step - 1, 0] + (HALF + 0.5)).astype(jnp.int32)
            low = (acc[1, part, :] * inv[step - 1, 1] + (HALF + 0.5)).astype(jnp.int32)
            send[c % 2, step - 1] = (high << 16) | low
            swap(c, step).start()
        acc[...] = jnp.zeros_like(acc)

    def scales():
        for step in range(1, groups):
            ext_to(step).wait_recv()
        for t in range(iters):
            for i in range(reps):
                part = slice(i * LANES, (i + 1) * LANES)
                count = ext[0, t, 0:1, part]
                for step in range(1, groups):
                    count = count + ext_recv[step - 1, t, 0:1, part]
                    scale[step - 1, t, part, :] = tall(ext_recv[step - 1, t, 4:5, part] / LEVELS)
                cnt[t, part, :] = tall(count)
        within[...] = jnp.zeros_like(within)

    def finish(c):
        load_prior(c).wait()
        for step in range(1, groups):
            swap(c, step).wait_recv()
        for i in range(reps):
            part = slice(i * LANES, (i + 1) * LANES)
            sums = [own[c, t, part, :] for t in range(iters)]
            for step in range(1, groups):
                for t, value in enumerate(decode(recv[c, step - 1, part, :])):
                    sums[t] = sums[t] + value * scale[step - 1, t, part, :]
            update(c, part, sums)

    def main_step(j, carry):
        c, k = j // chips, j % chips
        q = source(k)
        ahead = j + jnp.where(both > 0, chips + 2, 0)

        @pl.when((ahead >= jnp.where(both > 0, chips + 2, chips)) & (ahead < chunks * chips))
        def _():
            pull(ahead)

        from_partner(c, q).wait_recv()
        tally(c, q)
        late_step(j)

        @pl.when(k == chips - 1)
        def _():
            settle(c)

            @pl.when(c == 0)
            def _():
                scales()

            @pl.when(c > 0)
            def _():
                finish(c - 1)

        return carry

    lax.fori_loop(0, chunks * chips, main_step, 0)
    for x in range(late):
        finish_late(x)
    finish(chunks - 1)

    for i in range(reps):
        part = slice(i * LANES, (i + 1) * LANES)
        spread = jnp.sum(within[part, :].T, axis=0, keepdims=True)
        last = iters - 1
        count = ext[0, last, 0:1, part]
        square = ext[0, last, 1:2, part] + ext[0, last, 2:3, part] + ext[0, last, 3:4, part]
        for step in range(1, groups):
            far = ext_recv[step - 1, last, :, part]
            count = count + far[0:1]
            square = square + far[1:2] + far[2:3] + far[3:4]
        inertia[:, part] = (spread + square) / ((count + PRIOR) * features)

    for other in range(1, chips):
        meta_to(other).wait_send()
    for q in range(chips):
        meta_partner(q).wait_send()
    for step in range(1, groups):
        ext_to(step).wait_send()

    def drain(j, carry):
        c, q = j // chips, j % chips

        @pl.when((q <= chip) & (chip < chips - 1))
        def _():
            to_right(c, q).wait_send()

        @pl.when((q >= chip) & (chip > 0))
        def _():
            to_left(c, q).wait_send()

        to_partner(c, q).wait_send()
        return carry

    lax.fori_loop(0, chunks * chips, drain, 0)

    for x in range(late + 1):
        for step in range(1, groups):
            late_swap(x, step).wait_send()
        late_partner(x).wait_send()

        @pl.when(is_end)
        def _():
            late_inward(x).wait_send()

        @pl.when(jnp.logical_not(is_end))
        def _():
            late_share(x).wait_send()

    for x in range(late):

        @pl.when(jnp.logical_not(is_end))
        def _():
            for kind in range(3):
                for copy in late_codes(x, kind):
                    copy.wait_send()

    for c in range(chunks - 2, chunks):
        for step in range(1, groups):
            swap(c, step).wait_send()


def fused_buffers(local, block_rows, features, iters, owned, groups, shards):
    chips = shards // 2
    most = 2 * block_rows // shards
    width, late = LANES, features // LANES // 3
    chunks = features // LANES - late
    slots = CAP * most
    vmem = pltpu.VMEM
    f32, b16, i32 = jnp.float32, jnp.bfloat16, jnp.int32
    buffers = [
        ((chunks, shards, local, block_rows, width), b16),
        ((shards, local, META_ROWS, block_rows), b16),
        ((shards, local, iters * most, block_rows), b16),
        ((iters, chips, groups * owned, 2 * slots), b16),
        ((iters, groups * owned, width), f32),
        ((iters, groups, 2 * slots, width), b16),
        ((chunks, iters, owned, width), f32),
        ((2, groups - 1, owned, width), i32),
        ((chunks, groups - 1, owned, width), i32),
        ((groups - 1, iters, owned, width), f32),
        ((groups - 1, iters, owned, width), f32),
        ((iters, owned, width), f32),
        ((groups, iters, META_ROWS, owned), f32),
        ((groups - 1, iters, META_ROWS, owned), f32),
        ((chunks + late, owned, width), f32),
        ((owned, width), f32),
        ((META_ROWS, block_rows), f32),
        ((shards, local, groups * CAP, 16, LANES), b16),
        ((late, local, block_rows, width), b16),
        ((late, groups - 1, CAP, block_rows, width), b16),
        ((late, 4, groups, CAP, block_rows, width), b16),
        ((groups - 1, CAP, META_ROWS, block_rows), b16),
        ((4, groups, CAP, META_ROWS, block_rows), b16),
        ((groups, CAP, iters * most, block_rows), b16),
        ((iters, 1, groups * slots), i32),
        ((late, iters, groups * slots, width), b16),
        ((late, 4, iters, owned, width), f32),
        ((late, 3, owned, width), i32),
        ((late, 2, owned, width), i32),
        ((late, 3, 8, owned), f32),
        ((late, 2, 8, owned), f32),
    ]
    dma = pltpu.SemaphoreType.DMA
    sems = [dma((chunks,)), dma((chunks + late,))]
    sems += [dma((chips,))] * 4
    sems += [dma((chunks, chips))] * 6
    sems += [dma((groups - 1,))] * 2
    sems += [dma((chunks, groups - 1))] * 2
    sems += [dma((late,))] + [dma((late + 1, groups - 1))] * 2 + [dma((late + 1,))] * 6
    sems += [dma((late, 3)), dma((late, 2))] * 2
    return [vmem(s, d) for s, d in buffers], sems, buffers, most, chunks, late


def fits(local, block_rows, features, iters, owned, groups, shards):
    if features % LANES or features < 2 * LANES or owned % LANES or shards % 2:
        return False
    if shards != 8 or features < 6 * LANES:
        return False
    if iters != 2 or 4 * iters + FIXED > META_ROWS or (2 * block_rows) % shards:
        return False
    most = 2 * block_rows // shards
    if (CAP * most) % LANES or CAP * most > block_rows or most % 16 or block_rows % LANES:
        return False
    total = 0
    for shape, dtype in fused_buffers(local, block_rows, features, iters, owned, groups, shards)[2]:
        size = jnp.dtype(dtype).itemsize
        for extent in shape:
            size *= extent
        total += size
    return total < 60 * 2**20


def fused_body(embeddings, assignments, block_group, centroids):
    groups, shards = lax.axis_size("group"), lax.axis_size("shard")
    local, block_rows, features = embeddings.shape
    iters = assignments.shape[1]
    owned = centroids.shape[1] // shards
    buffers, sems, unused, most, chunks, late = fused_buffers(
        local, block_rows, features, iters, owned, groups, shards
    )

    out, inertia = pl.pallas_call(
        functools.partial(fused_kernel, chunks, late, most),
        out_shape=[
            pltpu.VMEM((owned, features), jnp.float32),
            pltpu.VMEM((1, owned), jnp.float32),
        ],
        in_specs=[
            pl.BlockSpec(memory_space=pltpu.SMEM),
            pl.BlockSpec(memory_space=pltpu.VMEM),
            pl.BlockSpec(memory_space=pl.ANY),
            pl.BlockSpec(memory_space=pl.ANY),
        ],
        out_specs=[pl.BlockSpec(memory_space=pltpu.VMEM)] * 2,
        scratch_shapes=buffers + sems,
        compiler_params=pltpu.CompilerParams(
            collective_id=0, has_side_effects=True, vmem_limit_bytes=61 * 2**20
        ),
    )(block_group, assignments, embeddings, centroids)
    return out[None], inertia


def choose(embeddings, assignments, block_group, centroids):
    groups, shards = lax.axis_size("group"), lax.axis_size("shard")
    local, block_rows, features = embeddings.shape
    owned = centroids.shape[1] // shards
    if fits(local, block_rows, features, assignments.shape[1], owned, groups, shards):
        return fused_body(embeddings, assignments, block_group, centroids)
    return body(embeddings, assignments, block_group, centroids)


def solution(mesh):
    in_specs = (
        P(("group", "shard"), None, None),
        P(("group", "shard"), None, None),
        P(("group", "shard")),
        P("group", None, None),
    )
    out_specs = (P("group", "shard", None), P("group", "shard"))
    return jax.shard_map(choose, mesh=mesh, in_specs=in_specs, out_specs=out_specs, check_vma=False)
```

```python
import functools

import jax
import jax.numpy as jnp
from jax import lax
from jax.experimental import pallas as pl
from jax.experimental.pallas import tpu as pltpu
from jax.sharding import PartitionSpec as P

PRIOR = 8.0
META = 8
CHUNKS = 3
MESH = pl.DeviceIdType.MESH


def exchange_kernel(n_gather, n_swap, width, column, *refs):
    n_in = n_gather + n_swap
    gathers, swaps = refs[:n_gather], refs[n_gather:n_in]
    outs = refs[n_in : 2 * n_in]
    gather_outs, swap_outs = outs[:n_gather], outs[n_gather:]
    scratch = refs[2 * n_in :]
    stages = scratch[:n_gather]
    scratch = scratch[n_gather:]

    groups, shards = lax.axis_size("group"), lax.axis_size("shard")
    chips = shards // 2
    mine, place = lax.axis_index("group"), lax.axis_index("shard")
    chip, core = place // 2, place % 2
    partner = (mine, chip * 2 + 1 - core)
    right = (mine, lax.rem(chip + 1, chips) * 2 + core)
    left = (mine, lax.rem(chip + chips - 1, chips) * 2 + core)

    def peer(step):
        return lax.rem(mine + step, groups)

    barrier = pltpu.get_barrier_semaphore()
    greeted = 0
    if n_gather:
        for device in (left, right, partner):
            pl.semaphore_signal(barrier, inc=1, device_id=device, device_id_type=MESH)
        greeted += 3
    if n_swap:
        for step in range(1, groups):
            pl.semaphore_signal(
                barrier, inc=1, device_id=(peer(step), place), device_id_type=MESH
            )
        greeted += groups - 1

    loads = []
    if n_gather:
        load_sem = scratch[0]
        for i in range(n_gather):
            source = gathers[i]
            if i == 0:
                source = source.at[:, :, pl.ds(column, width)]
            load = pltpu.make_async_copy(source, stages[i], load_sem.at[i])
            load.start()
            loads.append(load)
    pl.semaphore_wait(barrier, greeted)

    swap_copies = []
    if n_swap:
        swap_send, swap_recv = scratch[-2:]
        for step in range(1, groups):
            for i in range(n_swap):
                copy = pltpu.make_async_remote_copy(
                    src_ref=swaps[i].at[peer(step)],
                    dst_ref=swap_outs[i].at[step - 1],
                    send_sem=swap_send.at[i, step - 1],
                    recv_sem=swap_recv.at[i, step - 1],
                    device_id=(peer(step), place),
                    device_id_type=MESH,
                )
                copy.start()
                swap_copies.append(copy)

    if n_gather:
        store_sem, send_r, recv_r, send_l, recv_l, send_p, recv_p = scratch[1:8]
        stores = []

        def hop(i, source, origin, step, to, sends, recvs):
            return pltpu.make_async_remote_copy(
                src_ref=source,
                dst_ref=gather_outs[i].at[origin * 2 + core],
                send_sem=sends.at[i, step],
                recv_sem=recvs.at[i, step],
                device_id=to,
                device_id_type=MESH,
            )

        for i in range(n_gather):
            loads[i].wait()
            store = pltpu.make_async_copy(
                stages[i], gather_outs[i].at[place], store_sem.at[i]
            )

            @pl.when(chip < chips - 1)
            def _():
                hop(i, stages[i], chip, 0, right, send_r, recv_r).start()

            @pl.when(chip > 0)
            def _():
                hop(i, stages[i], chip, 0, left, send_l, recv_l).start()

            hop(i, stages[i], chip, chip, partner, send_p, recv_p).start()
            store.start()
            stores.append(store)

        for step in range(chips - 1):
            for i in range(n_gather):
                from_left = chip - 1 - step

                @pl.when(from_left >= 0)
                def _():
                    block = gather_outs[i].at[from_left * 2 + core]
                    hop(i, block, from_left, step, right, send_r, recv_r).wait_recv()

                    if step < chips - 2:

                        @pl.when(chip < chips - 1)
                        def _():
                            hop(i, block, from_left, step + 1, right, send_r, recv_r).start()

                    hop(i, block, from_left, from_left, partner, send_p, recv_p).start()

                from_right = chip + 1 + step

                @pl.when(from_right <= chips - 1)
                def _():
                    block = gather_outs[i].at[from_right * 2 + core]
                    hop(i, block, from_right, step, left, send_l, recv_l).wait_recv()

                    if step < chips - 2:

                        @pl.when(chip > 0)
                        def _():
                            hop(i, block, from_right, step + 1, left, send_l, recv_l).start()

                    hop(i, block, from_right, from_right, partner, send_p, recv_p).start()

        for i in range(n_gather):
            stores[i].wait()
            for step in range(chips - 1):

                @pl.when((chip - step >= 0) & (chip < chips - 1))
                def _():
                    hop(i, stages[i], chip, step, right, send_r, recv_r).wait_send()

                @pl.when((chip + step <= chips - 1) & (chip > 0))
                def _():
                    hop(i, stages[i], chip, step, left, send_l, recv_l).wait_send()

            for origin in range(chips):
                hop(i, stages[i], origin, origin, partner, send_p, recv_p).wait()

    for copy in swap_copies:
        copy.wait()


def exchange(gathers, swaps, width, column, key):
    groups, shards = lax.axis_size("group"), lax.axis_size("shard")
    chips = shards // 2
    n_gather, n_swap = len(gathers), len(swaps)
    shapes, scratch = [], []
    for i, array in enumerate(gathers):
        block = array.shape[:-1] + (width if i == 0 else array.shape[-1],)
        shapes.append(jax.ShapeDtypeStruct((shards,) + block, array.dtype))
        scratch.append(pltpu.VMEM(block, array.dtype))
    for array in swaps:
        shapes.append(jax.ShapeDtypeStruct((groups - 1,) + array.shape[1:], array.dtype))
    dma = pltpu.SemaphoreType.DMA
    if n_gather:
        scratch += [dma((n_gather,)), dma((n_gather,))]
        scratch += [dma((n_gather, max(chips - 1, 1)))] * 4
        scratch += [dma((n_gather, chips))] * 2
    if n_swap:
        scratch += [dma((n_swap, groups - 1))] * 2
    return pl.pallas_call(
        functools.partial(exchange_kernel, n_gather, n_swap, width, column),
        out_shape=shapes,
        in_specs=[pl.BlockSpec(memory_space=pl.ANY)] * (n_gather + n_swap),
        out_specs=[pl.BlockSpec(memory_space=pl.ANY)] * (n_gather + n_swap),
        scratch_shapes=scratch,
        compiler_params=pltpu.CompilerParams(collective_id=key, has_side_effects=True),
    )(*gathers, *swaps)


def tally_kernel(per_step, iters, with_extra, owners, labels, extra, rows, sums, *more):
    step = pl.program_id(0)
    centers = sums.shape[2]
    block_rows = rows.shape[1]

    @pl.when(step == 0)
    def _():
        sums[...] = jnp.zeros_like(sums)
        if with_extra:
            more[0][...] = jnp.zeros_like(more[0])

    ids = lax.broadcasted_iota(jnp.int32, (centers, block_rows), 0)
    for block in range(per_step):
        owner = owners[step * per_step + block]
        for t in range(iters):
            onehot = (ids == labels[block, t : t + 1, :]).astype(jnp.bfloat16)
            sums[owner, t] += jnp.dot(
                onehot, rows[block], preferred_element_type=jnp.float32
            )
            if with_extra:
                more[0][owner, t] += lax.dot_general(
                    extra[block],
                    onehot,
                    (((1,), (1,)), ((), ())),
                    preferred_element_type=jnp.float32,
                )


def tally(owners, labels, extra, rows, groups, centers, per_step, with_extra):
    blocks, iters, block_rows = labels.shape
    width = rows.shape[-1]
    shapes = [jax.ShapeDtypeStruct((groups, iters, centers, width), jnp.float32)]
    if with_extra:
        shapes.append(jax.ShapeDtypeStruct((groups, iters, extra.shape[1], centers), jnp.float32))
    out_specs = [pl.BlockSpec(s.shape, lambda i, o: (0, 0, 0, 0)) for s in shapes]
    return pl.pallas_call(
        functools.partial(tally_kernel, per_step, iters, with_extra),
        out_shape=shapes,
        grid_spec=pltpu.PrefetchScalarGridSpec(
            num_scalar_prefetch=1,
            grid=(blocks // per_step,),
            in_specs=[
                pl.BlockSpec((per_step, iters, block_rows), lambda i, o: (i, 0, 0)),
                pl.BlockSpec((per_step,) + extra.shape[1:], lambda i, o: (i, 0, 0)),
                pl.BlockSpec((per_step, block_rows, width), lambda i, o: (i, 0, 0)),
            ],
            out_specs=out_specs,
        ),
        compiler_params=pltpu.CompilerParams(vmem_limit_bytes=48 * 2**20),
    )(owners, labels, extra, rows)


def body(embeddings, assignments, block_group, centroids):
    groups, shards = lax.axis_size("group"), lax.axis_size("shard")
    mine, place = lax.axis_index("group"), lax.axis_index("shard")
    local, block_rows, features = embeddings.shape
    iters = assignments.shape[1]
    owned = centroids.shape[1] // shards
    chunks = CHUNKS if features % (CHUNKS * 128) == 0 else 1
    width = features // chunks
    blocks = shards * local

    wide = embeddings.astype(jnp.float32)
    squares = jnp.sum(wide * wide, axis=2)
    meta = jnp.concatenate(
        [
            assignments.astype(jnp.float32),
            jnp.broadcast_to(
                block_group[:, None, None].astype(jnp.float32), (local, 1, block_rows)
            ),
            squares[:, None, :],
            jnp.zeros((local, META - iters - 2, block_rows), jnp.float32),
        ],
        axis=1,
    )

    rows, metas = exchange([embeddings, meta], [], width, 0, 0)
    metas = metas.reshape(blocks, META, block_rows)
    labels = metas[:, :iters].astype(jnp.int32) - place * owned
    owners = metas[:, iters, 0].astype(jnp.int32)
    square = metas[:, iters + 1]
    high = lax.reduce_precision(square, 8, 7)
    middle = lax.reduce_precision(square - high, 8, 7)
    low = square - high - middle
    one = jnp.ones_like(square)
    zero = jnp.zeros_like(square)
    extra = jnp.stack([one, high, middle, low] + [zero] * 12, axis=1).astype(jnp.bfloat16)

    totals = []
    tail = None
    pending = []
    for chunk in range(chunks):
        result = tally(
            owners,
            labels,
            extra,
            rows.reshape(blocks, block_rows, width),
            groups,
            owned,
            local,
            chunk == 0,
        )
        column = (chunk + 1) * width
        if chunk + 1 < chunks:
            rows, *got = exchange([embeddings], result, width, column, chunk + 1)
        else:
            got = exchange([], result, width, 0, chunk + 1)
        whole = [
            lax.dynamic_index_in_dim(kept, mine, 0, keepdims=False) + jnp.sum(came, axis=0)
            for kept, came in zip(result, got)
        ]
        totals.append(whole[0])
        if chunk == 0:
            tail = whole[1]

    prior = lax.dynamic_slice_in_dim(centroids[0], place * owned, owned, 0)
    counts = tail[:, 0]
    within = tail[iters - 1, 1] + tail[iters - 1, 2] + tail[iters - 1, 3]
    pieces = []
    for chunk in range(chunks):
        previous = prior[:, chunk * width : (chunk + 1) * width]
        for t in range(iters):
            sums = totals[chunk][t]
            count = counts[t][:, None]
            if t == iters - 1:
                within = within + jnp.sum(
                    previous * (count * previous - 2.0 * sums), axis=1
                )
            previous = (sums + PRIOR * previous) / (count + PRIOR)
        pieces.append(previous)
    inertia = within / ((counts[iters - 1] + PRIOR) * features)
    return (jnp.concatenate(pieces, axis=1)[None], inertia[None])


LANES = 128
META_ROWS = 16
FIXED = 6
CAP = 2
LEVELS = 32000.0
HALF = 32768.0


def fused_kernel(
    chunks, late, most, owner_in, label_in, emb, cents, out, inertia,
    rows, metas, select, place_in, acc, compact, own, send, recv, inv, scale, cnt, ext,
    ext_recv, prior, within, lines, share,
    late_own, late_send, late_rows, late_meta_send, late_metas, late_select, late_cells, late_compact,
    late_acc, late_out, late_in, late_scale_out, late_scale_in,
    load_sem, prior_sem, meta_send, meta_recv, metap_send, metap_recv,
    send_r, recv_r, send_l, recv_l, send_p, recv_p, ext_ssem, ext_rsem, swap_send, swap_recv,
    late_load_sem, lswap_s, lswap_r, lpart_s, lpart_r, lin_s, lin_r, lshare_s, lshare_r,
    code_s, code_r, scale_s, scale_r,
):
    groups, shards = lax.axis_size("group"), lax.axis_size("shard")
    chips = shards // 2
    mine, place = lax.axis_index("group"), lax.axis_index("shard")
    chip, core = place // 2, place % 2
    partner = (mine, chip * 2 + 1 - core)
    right, left = (mine, place + 2), (mine, place - 2)
    is_end = (chip == 0) | (chip == chips - 1)
    mate = chip + 1 - 2 * lax.rem(chip, 2)
    targets = [place, (chips - 1 - chip) * 2 + core, (chips - 1 - mate) * 2 + core, mate * 2 + core]
    local, block_rows, features = emb.shape
    width = rows.shape[-1]
    iters = place_in.shape[0]
    owned = own.shape[2]
    slots = CAP * most
    reps = owned // LANES

    def peer(step):
        return (lax.rem(mine + step, groups), place)

    def remote(src, dst, ssem, rsem, to):
        return pltpu.make_async_remote_copy(
            src_ref=src, dst_ref=dst, send_sem=ssem, recv_sem=rsem,
            device_id=to, device_id_type=MESH,
        )

    def load(c):
        return pltpu.make_async_copy(
            emb.at[:, :, pl.ds(pl.multiple_of(c * width, width), width)],
            rows.at[c, place], load_sem.at[c],
        )

    def load_late(x):
        at = (chunks + x) * width
        return pltpu.make_async_copy(
            emb.at[:, :, pl.ds(at, width)], late_own.at[x], late_load_sem.at[x]
        )

    def load_prior(c):
        return pltpu.make_async_copy(
            cents.at[0, pl.ds(pl.multiple_of(place * owned, owned), owned),
                     pl.ds(pl.multiple_of(c * width, width), width)],
            prior.at[c], prior_sem.at[c],
        )

    for c in range(chunks):
        load(c).start()
    for x in range(late):
        load_late(x).start()

    barrier = pltpu.get_barrier_semaphore()
    for other in range(1, chips):
        pl.semaphore_signal(
            barrier, inc=1, device_id=(mine, lax.rem(chip + other, chips) * 2 + core),
            device_id_type=MESH,
        )
    pl.semaphore_signal(barrier, inc=1, device_id=partner, device_id_type=MESH)
    for step in range(1, groups):
        pl.semaphore_signal(barrier, inc=1, device_id=peer(step), device_id_type=MESH)
    pl.semaphore_wait(barrier, chips + groups - 1)

    def meta_to(other):
        target = lax.rem(chip + other, chips)
        return remote(
            metas.at[place], metas.at[place], meta_send.at[other], meta_recv.at[other],
            (mine, target * 2 + core),
        )

    def meta_partner(q):
        block = metas.at[q * 2 + core]
        return remote(block, block, metap_send.at[q], metap_recv.at[q], partner)

    def to_right(c, q):
        block = rows.at[c, q * 2 + core]
        return remote(block, block, send_r.at[c, chip - q], recv_r.at[c, chip - q], right)

    def to_left(c, q):
        block = rows.at[c, q * 2 + core]
        return remote(block, block, send_l.at[c, q - chip], recv_l.at[c, q - chip], left)

    def to_partner(c, q):
        block = rows.at[c, q * 2 + core]
        return remote(block, block, send_p.at[c, q], recv_p.at[c, q], partner)

    def from_left(c, q):
        block = rows.at[c, q * 2 + core]
        return remote(
            block, block, send_r.at[c, chip - 1 - q], recv_r.at[c, chip - 1 - q], right
        )

    def from_right(c, q):
        block = rows.at[c, q * 2 + core]
        return remote(
            block, block, send_l.at[c, q - chip - 1], recv_l.at[c, q - chip - 1], left
        )

    def from_partner(c, q):
        block = rows.at[c, q * 2 + 1 - core]
        return remote(block, block, send_p.at[c, q], recv_p.at[c, q], partner)

    def issue_own(c):
        @pl.when(chip < chips - 1)
        def _():
            to_right(c, chip).start()

        @pl.when(chip > 0)
        def _():
            to_left(c, chip).start()

        to_partner(c, chip).start()

    load(0).wait()
    load(1).wait()
    issue_own(0)
    for c in range(chunks + late):
        load_prior(c).start()
    for c in range(2, chunks):
        load(c).wait()
    for x in range(late):
        load_late(x).wait()

    ids_s = lax.broadcasted_iota(jnp.int32, (shards, block_rows), 0).astype(jnp.float32)
    before = (
        lax.broadcasted_iota(jnp.int32, (block_rows, block_rows), 0)
        < lax.broadcasted_iota(jnp.int32, (block_rows, block_rows), 1)
    ).astype(jnp.bfloat16)
    labels = [[label_in[b, t : t + 1, :].astype(jnp.float32) for t in range(iters)] for b in range(local)]
    ranges = [[jnp.floor((x + 0.5) * (1.0 / owned)) for x in xs] for xs in labels]
    hots = [[(ids_s == x).astype(jnp.float32) for x in xs] for xs in ranges]
    flat = [x for xs in hots for x in xs]
    earlier = jnp.dot(
        jnp.concatenate(flat, axis=0).astype(jnp.bfloat16), before,
        preferred_element_type=jnp.float32,
    )
    lines[...] = jnp.zeros_like(lines)
    for b in range(local):
        total = jnp.zeros((block_rows, width), jnp.float32)
        top = jnp.zeros((block_rows, width), jnp.float32)
        for c in range(chunks + late):
            x = rows[c, place, b] if c < chunks else late_own[c - chunks, b]
            x = x.astype(jnp.float32)
            total = total + x * x
            top = jnp.maximum(top, jnp.abs(x))
        square = jnp.sum(total.T, axis=0, keepdims=True)
        high = square.astype(jnp.bfloat16).astype(jnp.float32)
        middle = (square - high).astype(jnp.bfloat16).astype(jnp.float32)
        lines[0:1, :] = jnp.ones_like(square)
        lines[1:2, :] = high
        lines[2:3, :] = middle
        lines[3:4, :] = square - high - middle
        lines[4:5, :] = jnp.max(top.T, axis=0, keepdims=True)
        turn = owner_in[b] * CAP
        for other in range(b):
            turn = turn + jnp.where(owner_in[other] == owner_in[b], 1, 0)
        lines[5:6, :] = jnp.full((1, block_rows), turn, jnp.int32).astype(jnp.float32)
        for t in range(iters):
            base = FIXED + 4 * t
            inside = labels[b][t] - ranges[b][t] * owned
            coarse = jnp.floor((inside + 0.5) * (1.0 / 256))
            at = (b * iters + t) * shards
            lines[base : base + 1, :] = inside - 256.0 * coarse
            lines[base + 1 : base + 2, :] = coarse
            lines[base + 2 : base + 3, :] = ranges[b][t]
            lines[base + 3 : base + 4, :] = jnp.sum(
                hots[b][t] * earlier[at : at + shards, :], axis=0, keepdims=True
            )
        metas[place, b] = lines[...].astype(jnp.bfloat16)

    for other in range(1, chips):
        meta_to(other).start()
    issue_own(1)

    @pl.when(is_end)
    def _():
        for c in range(2, chunks):
            issue_own(c)

    def late_swap(x, step):
        sent = late_meta_send if x == late else late_send.at[x]
        kept = late_metas if x == late else late_rows.at[x]
        return remote(
            sent.at[step - 1], kept.at[core, step], lswap_s.at[x, step - 1],
            lswap_r.at[x, step - 1], peer(step),
        )

    def late_block(x, at):
        return late_metas.at[at] if x == late else late_rows.at[x, at]

    def late_partner(x):
        block = late_block(x, core)
        return remote(block, block, lpart_s.at[x], lpart_r.at[x], partner)

    def late_inward(x):
        return remote(
            late_block(x, core), late_block(x, 2 + core), lin_s.at[x], lin_r.at[x],
            (mine, mate * 2 + core),
        )

    def late_share(x):
        block = late_block(x, 2 + core)
        return remote(block, block, lshare_s.at[x], lshare_r.at[x], partner)

    def late_start():
        for x in (late,) + tuple(range(late)):
            for step in range(1, groups):
                late_swap(x, step).wait_recv()
            late_partner(x).start()

            @pl.when(is_end)
            def _():
                late_inward(x).start()

    chosen = []
    for b in range(local):
        turn = metas[place, b].astype(jnp.float32)[5:6, :LANES].astype(jnp.int32) - mine * CAP
        chosen.append(jnp.where(turn < 0, turn + groups * CAP, turn))
    for step in range(groups):
        for i in range(CAP):
            weights = [
                jnp.broadcast_to(
                    (turn == step * CAP + i).astype(jnp.float32), (META_ROWS, LANES)
                ).astype(jnp.bfloat16)
                for turn in chosen
            ]

            def pick(blocks):
                tiles = [x.reshape(x.shape[0] // META_ROWS, META_ROWS, LANES) for x in blocks]
                put = tiles[0] * weights[0][None]
                for b in range(1, local):
                    put = put + tiles[b] * weights[b][None]
                return put.reshape(blocks[0].shape)

            for lane in range(0, block_rows, LANES):
                part = slice(lane, lane + LANES)
                put = pick([metas[place, b, :, part] for b in range(local)])
                if step == 0:
                    late_metas[core, 0, i, :, part] = put
                else:
                    late_meta_send[step - 1, i, :, part] = put
            for x in range(late):
                put = pick([late_own[x, b] for b in range(local)])
                if step == 0:
                    late_rows[x, core, 0, i] = put
                else:
                    late_send[x, step - 1, i] = put
    for x in (late,) + tuple(range(late)):
        for step in range(1, groups):
            late_swap(x, step).start()

    on_left, on_right = chip, chips - 1 - chip
    both = jnp.minimum(on_left, on_right)

    def source(k):
        paired = k <= 2 * both
        distance = jnp.where(paired, (k + 1) // 2, k - both)
        is_left = jnp.where(paired, (k % 2) == 1, on_left > on_right)
        return jnp.where(is_left, chip - distance, chip + distance)

    def pull(j):
        c, k = j // chips, j % chips
        q = source(k)

        @pl.when((k == 0) & (c + 2 < chunks) & jnp.logical_not(is_end))
        def _():
            issue_own(c + 2)

        @pl.when(q < chip)
        def _():
            from_left(c, q).wait_recv()

            @pl.when(chip < chips - 1)
            def _():
                to_right(c, q).start()

            to_partner(c, q).start()

        @pl.when(q > chip)
        def _():
            from_right(c, q).wait_recv()

            @pl.when(chip > 0)
            def _():
                to_left(c, q).start()

            to_partner(c, q).start()

    ids_m = lax.rem(lax.broadcasted_iota(jnp.int32, (slots, block_rows), 0), most)
    ids_c = lax.broadcasted_iota(jnp.int32, (owned, slots), 0)
    turns = lax.broadcasted_iota(jnp.int32, (1, slots), 1) // most

    ext[...] = jnp.zeros_like(ext)
    acc[...] = jnp.zeros_like(acc)
    late_acc[...] = jnp.zeros_like(late_acc)
    late_scale_out[...] = jnp.zeros_like(late_scale_out)

    def take_meta(q, core_of):
        origin = q * 2 + core_of
        rel = []
        for b in range(local):
            place_of = metas[origin, b].astype(jnp.float32)[5:6, :slots].astype(jnp.int32) - mine * CAP
            rel.append(jnp.where(place_of < 0, place_of + groups * CAP, place_of))
            for i in range(groups * CAP):
                one = (rel[b] == i).astype(jnp.float32)[:, :LANES]
                share[origin, b, i] = jnp.broadcast_to(one, (16, LANES)).astype(jnp.bfloat16)
        for t in range(iters):
            base = FIXED + 4 * t
            found = []
            for b in range(local):
                e = metas[origin, b]
                f = e.astype(jnp.float32)
                wanted = f[base + 2 : base + 3, :].astype(jnp.int32) == place
                pos = jnp.where(wanted, f[base + 3 : base + 4, :].astype(jnp.int32), -1)
                hot = (ids_m == pos).astype(jnp.bfloat16)
                select[origin, b, t * most : (t + 1) * most, :] = hot[:most, :]
                found.append(
                    lax.dot_general(
                        e, hot, (((1,), (1,)), ((), ())), preferred_element_type=jnp.float32
                    )
                )
            for g in range(groups):
                pair = jnp.zeros((META_ROWS, slots), jnp.float32)
                for b in range(local):
                    pair = pair + jnp.where(rel[b] == turns + g * CAP, found[b], 0.0)
                label = pair[base : base + 1, :] + 256.0 * pair[base + 1 : base + 2, :]
                cell = jnp.where(pair[0:1, :] > 0.5, label.astype(jnp.int32), -1)
                hot = (ids_c == cell).astype(jnp.bfloat16)
                part = slice(core_of * slots, (core_of + 1) * slots)
                place_in[t, q, g * owned : (g + 1) * owned, part] = hot
                ext[g, t] += lax.dot_general(
                    pair.astype(jnp.bfloat16), hot, (((1,), (1,)), ((), ())),
                    preferred_element_type=jnp.float32,
                )

    def meta_step(k, carry):
        q = source(k)

        @pl.when(q != chip)
        def _():
            other = lax.rem(chip - q + chips, chips)
            block = metas.at[q * 2 + core]
            remote(block, block, meta_send.at[other], meta_recv.at[other], left).wait_recv()

        meta_partner(q).start()
        for core_of in range(2):

            @pl.when(core_of != core)
            def _():
                block = metas.at[q * 2 + 1 - core]
                remote(block, block, metap_send.at[q], metap_recv.at[q], partner).wait_recv()

        for core_of in range(2):
            take_meta(q, core_of)
        pull(k)

        @pl.when((both > 0) & (k >= chips - 2))
        def _():
            pull(k + 2)

        return carry

    lax.fori_loop(0, chips, meta_step, 0)
    late_start()

    def ext_to(step):
        return remote(
            ext.at[step], ext_recv.at[step - 1], ext_ssem.at[step - 1], ext_rsem.at[step - 1],
            peer(step),
        )

    for step in range(1, groups):
        ext_to(step).start()

    def tall(row):
        return jnp.broadcast_to(row, (LANES, LANES)).T

    for step in range(1, groups):
        for t in range(iters):
            for i in range(reps):
                bound = ext[step, t, 4:5, i * LANES : (i + 1) * LANES]
                inv[step - 1, t, i * LANES : (i + 1) * LANES, :] = tall(
                    LEVELS / jnp.maximum(bound, 1e-30)
                )

    def swap(c, step):
        return remote(
            send.at[c % 2, step - 1], recv.at[c, step - 1], swap_send.at[c, step - 1],
            swap_recv.at[c, step - 1], peer(step),
        )

    tile = owned

    def gather_slots(c, q):
        for core_of in range(2):
            origin = q * 2 + core_of
            got = []
            for b in range(local):
                x = jnp.dot(select[origin, b], rows[c, origin, b], preferred_element_type=jnp.float32)
                got.append(x.astype(jnp.bfloat16).reshape(iters * most // 16, 16, width))
            for g in range(groups):
                for i in range(CAP):
                    put = got[0] * share[origin, 0, g * CAP + i][None]
                    for b in range(1, local):
                        put = put + got[b] * share[origin, b, g * CAP + i][None]
                    put = put.reshape(iters, most, width)
                    at = core_of * slots + i * most
                    for t in range(iters):
                        compact[t, g, at : at + most, :] = put[t]

    def tally(c, q):
        gather_slots(c, q)

        def body(i, carry):
            for t in range(iters):
                part = pl.ds(pl.multiple_of(i * tile, tile), tile)
                acc[t, part, :] += jnp.dot(
                    place_in[t, q, part, :], compact[t, i], preferred_element_type=jnp.float32
                )
            return carry

        lax.fori_loop(0, groups, body, 0, unroll=True)

    def decode(word):
        high = lax.shift_right_logical(word, 16)
        low = word & 0xFFFF
        return [high.astype(jnp.float32) - HALF, low.astype(jnp.float32) - HALF]

    def late_codes(x, kind):
        to = mate if kind == 2 else chips - 1 - chip
        slot = 0 if kind == 2 else kind
        device = (mine, to * 2 + core)
        return (
            remote(late_out.at[x, kind], late_in.at[x, slot], code_s.at[x, kind], code_r.at[x, slot], device),
            remote(
                late_scale_out.at[x, kind], late_scale_in.at[x, slot], scale_s.at[x, kind],
                scale_r.at[x, slot], device,
            ),
        )

    ones = jnp.ones((LANES, LANES), jnp.bfloat16)

    def late_emit(x, kind, sums_of):
        for i in range(reps):
            part = slice(i * LANES, (i + 1) * LANES)
            codes = []
            for t, value in enumerate(sums_of(part)):
                power = (value * value * 1.02).astype(jnp.bfloat16)
                tall_norm = jnp.dot(power, ones, preferred_element_type=jnp.float32)
                wide_norm = lax.dot_general(
                    ones[:16], power, (((1,), (1,)), ((), ())), preferred_element_type=jnp.float32
                )
                late_scale_out[x, kind, t : t + 1, part] = (
                    jnp.sqrt(jnp.maximum(wide_norm[0:1], 1e-30)) * (1.0 / LEVELS)
                )
                inverse = LEVELS * lax.rsqrt(jnp.maximum(tall_norm, 1e-30))
                codes.append((value * inverse + (HALF + 0.5)).astype(jnp.int32))
            late_out[x, kind, part, :] = (codes[0] << 16) | codes[1]
        for copy in late_codes(x, kind):
            copy.start()

    def late_wait(x, slot):
        for copy in (
            remote(late_out.at[x, slot], late_in.at[x, slot], code_s.at[x, slot], code_r.at[x, slot], partner),
            remote(
                late_scale_out.at[x, slot], late_scale_in.at[x, slot], scale_s.at[x, slot],
                scale_r.at[x, slot], partner,
            ),
        ):
            copy.wait_recv()

    def late_sums(x, target, slot, part):
        values = decode(late_in[x, slot, part, :])
        return [
            late_acc[x, target, t, part, :] + v * tall(late_scale_in[x, slot, t : t + 1, part])
            for t, v in enumerate(values)
        ]

    ids_w = lax.broadcasted_iota(jnp.int32, (owned, groups * slots), 0)

    def late_tally(target, wanted_range, at):
        for t in range(iters):
            base = FIXED + 4 * t
            for g in range(groups):
                found = []
                for i in range(CAP):
                    e = late_metas[at, g, i]
                    f = e.astype(jnp.float32)
                    wanted = (f[base + 2 : base + 3, :].astype(jnp.int32) == wanted_range) & (f[0:1, :] > 0.5)
                    pos = jnp.where(wanted, f[base + 3 : base + 4, :].astype(jnp.int32), -1)
                    hot = (ids_m == pos).astype(jnp.bfloat16)
                    late_select[g, i, t * most : (t + 1) * most, :] = hot[:most, :]
                    x = lax.dot_general(
                        e, hot, (((1,), (1,)), ((), ())), preferred_element_type=jnp.float32
                    )
                    found.append(jnp.where(turns == i, x, 0.0))
                pair = found[0]
                for x in found[1:]:
                    pair = pair + x
                label = pair[base : base + 1, :] + 256.0 * pair[base + 1 : base + 2, :]
                late_cells[t, :, g * slots : (g + 1) * slots] = jnp.where(
                    pair[0:1, :] > 0.5, label.astype(jnp.int32), -1
                )
        for x in range(late):
            for g in range(groups):
                for i in range(CAP):
                    got = jnp.dot(
                        late_select[g, i], late_rows[x, at, g, i], preferred_element_type=jnp.float32
                    ).astype(jnp.bfloat16)
                    spot = g * slots + i * most
                    for t in range(iters):
                        late_compact[x, t, spot : spot + most, :] = got[t * most : (t + 1) * most, :]
        for t in range(iters):
            hot = (ids_w == late_cells[t]).astype(jnp.bfloat16)
            for x in range(late):
                late_acc[x, target, t] += jnp.dot(
                    hot, late_compact[x, t], preferred_element_type=jnp.float32
                )

    def late_run(j, codes):
        code_of = jnp.int32(codes[0])
        for i, entry in enumerate(codes):
            code_of = jnp.where(j == i, entry, code_of)
        target, at = code_of // 4, code_of % 4
        wanted_range = targets[0]
        for i in range(1, 4):
            wanted_range = jnp.where(target == i, targets[i], wanted_range)
        here = jnp.where(is_end, (target == 0) & (at < 2), True)

        @pl.when(here & (j < len(codes)))
        def _():
            late_tally(target, wanted_range, at)

    def late_step(j):
        @pl.when(j == 0)
        def _():
            for x in range(late + 1):
                late_partner(x).wait_recv()

        @pl.when((j == 8) & jnp.logical_not(is_end))
        def _():
            for x in range(late + 1):
                late_inward(x).wait_recv()
                late_share(x).start()
            for x in range(late + 1):
                late_share(x).wait_recv()

        late_run(j, (8, 9, 4, 5, 12, 13, 0, 1, 10, 11, 6, 7))

        for kind, when in ((1, 9), (0, 11)):

            @pl.when((j == when) & jnp.logical_not(is_end))
            def _():
                for x in range(late):
                    late_emit(
                        x, kind, lambda part: [late_acc[x, kind + 1, t, part, :] for t in range(iters)]
                    )

        @pl.when((j == 14) & jnp.logical_not(is_end))
        def _():
            for x in range(late):
                late_wait(x, 1)
                late_emit(x, 2, lambda part: late_sums(x, 3, 1, part))

    def finish_late(x):
        load_prior(chunks + x).wait()
        late_wait(x, 0)
        for i in range(reps):
            part = slice(i * LANES, (i + 1) * LANES)
            update(chunks + x, part, late_sums(x, 0, 0, part))

    def update(c, part, sums):
        previous = prior[c, part, :]
        for t in range(iters):
            count = cnt[t, part, :]
            if t == iters - 1:
                within[part, :] += previous * (count * previous - 2.0 * sums[t])
            previous = (sums[t] + PRIOR * previous) / (count + PRIOR)
        at = c * width
        out[part, pl.ds(at if isinstance(at, int) else pl.multiple_of(at, width), width)] = previous

    def settle(c):
        for t in range(iters):
            own[c, t] = acc[t, :owned, :]

        @pl.when(c >= 2)
        def _():
            for step in range(1, groups):
                swap(c - 2, step).wait_send()

        for step in range(1, groups):
            part = slice(step * owned, (step + 1) * owned)
            high = (acc[0, part, :] * inv[step - 1, 0] + (HALF + 0.5)).astype(jnp.int32)
            low = (acc[1, part, :] * inv[step - 1, 1] + (HALF + 0.5)).astype(jnp.int32)
            send[c % 2, step - 1] = (high << 16) | low
            swap(c, step).start()
        acc[...] = jnp.zeros_like(acc)

    def scales():
        for step in range(1, groups):
            ext_to(step).wait_recv()
        for t in range(iters):
            for i in range(reps):
                part = slice(i * LANES, (i + 1) * LANES)
                count = ext[0, t, 0:1, part]
                for step in range(1, groups):
                    count = count + ext_recv[step - 1, t, 0:1, part]
                    scale[step - 1, t, part, :] = tall(ext_recv[step - 1, t, 4:5, part] / LEVELS)
                cnt[t, part, :] = tall(count)
        within[...] = jnp.zeros_like(within)

    def finish(c):
        load_prior(c).wait()
        for step in range(1, groups):
            swap(c, step).wait_recv()
        for i in range(reps):
            part = slice(i * LANES, (i + 1) * LANES)
            sums = [own[c, t, part, :] for t in range(iters)]
            for step in range(1, groups):
                for t, value in enumerate(decode(recv[c, step - 1, part, :])):
                    sums[t] = sums[t] + value * scale[step - 1, t, part, :]
            update(c, part, sums)

    def main_step(j, carry):
        c, k = j // chips, j % chips
        q = source(k)
        ahead = j + jnp.where(both > 0, chips + 2, 0)

        @pl.when((ahead >= jnp.where(both > 0, chips + 2, chips)) & (ahead < chunks * chips))
        def _():
            pull(ahead)

        from_partner(c, q).wait_recv()
        tally(c, q)
        late_step(j)

        @pl.when(k == chips - 1)
        def _():
            settle(c)


        return carry

    lax.fori_loop(0, chunks * chips, main_step, 0)
    def late_rest(j, carry):
        late_run(j, (2, 3))
        return carry

    lax.fori_loop(0, 2, late_rest, 0)
    scales()
    for c in range(chunks - 1):
        finish(c)
    for x in range(late):
        finish_late(x)
    finish(chunks - 1)

    for i in range(reps):
        part = slice(i * LANES, (i + 1) * LANES)
        spread = jnp.sum(within[part, :].T, axis=0, keepdims=True)
        last = iters - 1
        count = ext[0, last, 0:1, part]
        square = ext[0, last, 1:2, part] + ext[0, last, 2:3, part] + ext[0, last, 3:4, part]
        for step in range(1, groups):
            far = ext_recv[step - 1, last, :, part]
            count = count + far[0:1]
            square = square + far[1:2] + far[2:3] + far[3:4]
        inertia[:, part] = (spread + square) / ((count + PRIOR) * features)

    for other in range(1, chips):
        meta_to(other).wait_send()
    for q in range(chips):
        meta_partner(q).wait_send()
    for step in range(1, groups):
        ext_to(step).wait_send()

    def drain(j, carry):
        c, q = j // chips, j % chips

        @pl.when((q <= chip) & (chip < chips - 1))
        def _():
            to_right(c, q).wait_send()

        @pl.when((q >= chip) & (chip > 0))
        def _():
            to_left(c, q).wait_send()

        to_partner(c, q).wait_send()
        return carry

    lax.fori_loop(0, chunks * chips, drain, 0)

    for x in range(late + 1):
        for step in range(1, groups):
            late_swap(x, step).wait_send()
        late_partner(x).wait_send()

        @pl.when(is_end)
        def _():
            late_inward(x).wait_send()

        @pl.when(jnp.logical_not(is_end))
        def _():
            late_share(x).wait_send()

    for x in range(late):

        @pl.when(jnp.logical_not(is_end))
        def _():
            for kind in range(3):
                for copy in late_codes(x, kind):
                    copy.wait_send()

    for c in range(chunks - 2, chunks):
        for step in range(1, groups):
            swap(c, step).wait_send()


def fused_buffers(local, block_rows, features, iters, owned, groups, shards):
    chips = shards // 2
    most = 2 * block_rows // shards
    width, late = LANES, features // LANES // 3
    chunks = features // LANES - late
    slots = CAP * most
    vmem = pltpu.VMEM
    f32, b16, i32 = jnp.float32, jnp.bfloat16, jnp.int32
    buffers = [
        ((chunks, shards, local, block_rows, width), b16),
        ((shards, local, META_ROWS, block_rows), b16),
        ((shards, local, iters * most, block_rows), b16),
        ((iters, chips, groups * owned, 2 * slots), b16),
        ((iters, groups * owned, width), f32),
        ((iters, groups, 2 * slots, width), b16),
        ((chunks, iters, owned, width), f32),
        ((2, groups - 1, owned, width), i32),
        ((chunks, groups - 1, owned, width), i32),
        ((groups - 1, iters, owned, width), f32),
        ((groups - 1, iters, owned, width), f32),
        ((iters, owned, width), f32),
        ((groups, iters, META_ROWS, owned), f32),
        ((groups - 1, iters, META_ROWS, owned), f32),
        ((chunks + late, owned, width), f32),
        ((owned, width), f32),
        ((META_ROWS, block_rows), f32),
        ((shards, local, groups * CAP, 16, LANES), b16),
        ((late, local, block_rows, width), b16),
        ((late, groups - 1, CAP, block_rows, width), b16),
        ((late, 4, groups, CAP, block_rows, width), b16),
        ((groups - 1, CAP, META_ROWS, block_rows), b16),
        ((4, groups, CAP, META_ROWS, block_rows), b16),
        ((groups, CAP, iters * most, block_rows), b16),
        ((iters, 1, groups * slots), i32),
        ((late, iters, groups * slots, width), b16),
        ((late, 4, iters, owned, width), f32),
        ((late, 3, owned, width), i32),
        ((late, 2, owned, width), i32),
        ((late, 3, 8, owned), f32),
        ((late, 2, 8, owned), f32),
    ]
    dma = pltpu.SemaphoreType.DMA
    sems = [dma((chunks,)), dma((chunks + late,))]
    sems += [dma((chips,))] * 4
    sems += [dma((chunks, chips))] * 6
    sems += [dma((groups - 1,))] * 2
    sems += [dma((chunks, groups - 1))] * 2
    sems += [dma((late,))] + [dma((late + 1, groups - 1))] * 2 + [dma((late + 1,))] * 6
    sems += [dma((late, 3)), dma((late, 2))] * 2
    return [vmem(s, d) for s, d in buffers], sems, buffers, most, chunks, late


def fits(local, block_rows, features, iters, owned, groups, shards):
    if features % LANES or features < 2 * LANES or owned % LANES or shards % 2:
        return False
    if shards != 8 or features < 6 * LANES:
        return False
    if iters != 2 or 4 * iters + FIXED > META_ROWS or (2 * block_rows) % shards:
        return False
    most = 2 * block_rows // shards
    if (CAP * most) % LANES or CAP * most > block_rows or most % 16 or block_rows % LANES:
        return False
    total = 0
    for shape, dtype in fused_buffers(local, block_rows, features, iters, owned, groups, shards)[2]:
        size = jnp.dtype(dtype).itemsize
        for extent in shape:
            size *= extent
        total += size
    return total < 60 * 2**20


def fused_body(embeddings, assignments, block_group, centroids):
    groups, shards = lax.axis_size("group"), lax.axis_size("shard")
    local, block_rows, features = embeddings.shape
    iters = assignments.shape[1]
    owned = centroids.shape[1] // shards
    buffers, sems, unused, most, chunks, late = fused_buffers(
        local, block_rows, features, iters, owned, groups, shards
    )

    out, inertia = pl.pallas_call(
        functools.partial(fused_kernel, chunks, late, most),
        out_shape=[
            pltpu.VMEM((owned, features), jnp.float32),
            pltpu.VMEM((1, owned), jnp.float32),
        ],
        in_specs=[
            pl.BlockSpec(memory_space=pltpu.SMEM),
            pl.BlockSpec(memory_space=pltpu.VMEM),
            pl.BlockSpec(memory_space=pl.ANY),
            pl.BlockSpec(memory_space=pl.ANY),
        ],
        out_specs=[pl.BlockSpec(memory_space=pltpu.VMEM)] * 2,
        scratch_shapes=buffers + sems,
        compiler_params=pltpu.CompilerParams(
            collective_id=0, has_side_effects=True, vmem_limit_bytes=61 * 2**20
        ),
    )(block_group, assignments, embeddings, centroids)
    return out[None], inertia


def choose(embeddings, assignments, block_group, centroids):
    groups, shards = lax.axis_size("group"), lax.axis_size("shard")
    local, block_rows, features = embeddings.shape
    owned = centroids.shape[1] // shards
    if fits(local, block_rows, features, assignments.shape[1], owned, groups, shards):
        return fused_body(embeddings, assignments, block_group, centroids)
    return body(embeddings, assignments, block_group, centroids)


def solution(mesh):
    in_specs = (
        P(("group", "shard"), None, None),
        P(("group", "shard"), None, None),
        P(("group", "shard")),
        P("group", None, None),
    )
    out_specs = (P("group", "shard", None), P("group", "shard"))
    return jax.shard_map(choose, mesh=mesh, in_specs=in_specs, out_specs=out_specs, check_vma=False)
```
